32 devices in a mesh: seq: 8 (over z, core), tp: 4 (over y, x).
Axes of the slice: x: 2, y: 2, z: 4, core: 2. Of those that a mesh axis runs over, the one named last changes fastest.
Arguments:
- tokens: bfloat16 [1024, 8192], P('seq'), may hold values from -6 to 6
- conv_weight: float32 [4, 8192], replicated, may hold values from -3 to 3
- norm_gain: float32 [8192], replicated, may hold values from 0.25 to 1.75
- gate_weight: bfloat16 [8192, 14336], P('seq', 'tp'), may hold values from -0.0625 to 0.0625
- up_weight: bfloat16 [8192, 14336], P('seq', 'tp'), may hold values from -0.0625 to 0.0625
- down_weight: bfloat16 [14336, 8192], P('tp', 'seq'), may hold values from -0.046875 to 0.046875
Outputs:
- mixed_out: bfloat16 [1024, 8192], P(('seq', 'tp'))
The draws below stay inside these ranges and needn't reach their ends.
All inputs are finite; a program needn't handle non-finite values.
Results may differ from the reference program's by a relative error of at most 0.03.
Values may be sent and summed in bfloat16 or wider, within the bound.
A program may use at most 128 MiB of HBM per device.

```python
import jax
import jax.numpy as jnp
from jax import lax

D = 8192
FF = 14336
TAPS = 4
TOKENS = 1024
N_SEQ = 8


def levels(key, dims, cuts, low, largest):
    def one(axis_at, parts):
        steps = jax.random.uniform(jax.random.fold_in(jax.random.fold_in(key, 6), axis_at), (parts,), jnp.float32, low / len(cuts), largest / len(cuts))
        return jnp.repeat(jnp.exp(steps), dims[axis_at] // parts).reshape((-1,) + (1,) * (len(dims) - axis_at - 1))

    loudness = one(*cuts[0])
    for cut in cuts[1:]:
        loudness = loudness * one(*cut)
    return loudness


def scatter_about(key, dims, deviation, limit, split=(), dtype=jnp.bfloat16):
    array = deviation * jax.random.normal(key, dims, jnp.float32)
    if split:
        array = array * levels(key, dims, split, -0.22, 0.18)
    return jnp.clip(array, -limit, limit).astype(dtype)


def setup_inputs(seed: int = 0) -> dict:
    keys = jax.random.split(jax.random.key(seed), 7)
    return {
        "tokens": scatter_about(keys[0], (TOKENS, D), 1.0, 6.0, ((0, 8),)),
        "conv_weight": scatter_about(keys[1], (TAPS, D), 0.5, 3.0, (), jnp.float32),
        "norm_gain": jnp.clip(1.0 + 0.15 * jax.random.normal(keys[2], (D,), jnp.float32), 0.25, 1.75),
        "gate_weight": scatter_about(keys[3], (D, FF), D ** -0.5, 0.0625, ((0, 8), (1, 4))),
        "up_weight": scatter_about(keys[4], (D, FF), D ** -0.5, 0.0625, ((0, 8), (1, 4))),
        "down_weight": scatter_about(keys[5], (FF, D), FF ** -0.5, 0.046875, ((0, 4), (1, 8))),
    }


def reference(tokens, conv_weight, norm_gain, gate_weight, up_weight, down_weight):
    inputs = tokens.astype(jnp.float32)
    tok_count = inputs.shape[0]
    model_width = inputs.shape[1]
    taps_count = conv_weight.shape[0]
    padded = jnp.concatenate([jnp.zeros((taps_count - 1, model_width), jnp.float32), inputs], 0)
    conv_out = jnp.zeros((tok_count, model_width), jnp.float32)
    for tap_index in range(taps_count):
        begin = taps_count - 1 - tap_index
        conv_out = conv_out + conv_weight[tap_index][None, :] * padded[begin:begin + tok_count]
    scale_rms = lax.rsqrt(lax.optimization_barrier(jnp.mean(conv_out * conv_out, axis=-1, keepdims=True)) + 1e-05)
    normed = (conv_out * scale_rms * norm_gain[None, :]).astype(jnp.bfloat16)
    group_width = model_width // N_SEQ
    hidden_width = gate_weight.shape[1]
    gate = jnp.zeros((tok_count, hidden_width), jnp.float32)
    up_sum = jnp.zeros((tok_count, hidden_width), jnp.float32)
    for group_index in range(N_SEQ):
        lower = group_index * group_width
        feats = normed[:, lower:lower + group_width]
        gate_part = jnp.dot(feats, gate_weight[lower:lower + group_width], preferred_element_type=jnp.float32)
        up_part = jnp.dot(feats, up_weight[lower:lower + group_width], preferred_element_type=jnp.float32)
        gate = gate + lax.optimization_barrier(gate_part.astype(jnp.bfloat16)).astype(jnp.float32)
        up_sum = up_sum + lax.optimization_barrier(up_part.astype(jnp.bfloat16)).astype(jnp.float32)
    hidden = (jax.nn.silu(gate) * up_sum).astype(jnp.bfloat16)
    return jnp.dot(hidden, down_weight, preferred_element_type=jnp.float32).astype(jnp.bfloat16)
```

```python
import functools

import jax
import jax.numpy as jnp
from jax import lax
from jax.experimental import pallas as pl
from jax.experimental.pallas import tpu as pltpu
from jax.sharding import PartitionSpec as P

MESH = pl.DeviceIdType.MESH
WIDTH = 128
RS_LAG = 2
AG_LAG = 2
SOURCE_LEAD = 10
RELAY_LEAD = 4
PARTNER_LEAD = 1
OUT_LAG = 3


def from_behind(shard, axis, by):
    peers = lax.axis_size(axis)
    pairs = [(i, i + by) for i in range(peers) if 0 <= i + by < peers]
    return lax.ppermute(shard, axis, pairs)


def ffn_kernel(seq_n, tp_n, x_ref, gw_ref, uw_ref, dw_ref, out_ref,
               x_all, w_buf, d_buf, chain, hid, part, acc, stage, got, fin, rows_out,
               w_sem, w_snd, w_rcv, d_sem, z_snd, z_rcv, t_snd, t_rcv, p_snd, p_rcv,
               c_snd, c_rcv, h_snd, h_rcv, q_snd, q_rcv, s_snd, s_rcv, f_snd, f_rcv):
    stops = seq_n // 2
    groups = seq_n // 2
    seq_i = lax.axis_index("seq")
    tp_i = lax.axis_index("tp")
    pos = seq_i // 2
    core = seq_i % 2
    partner = (pos * 2 + 1 - core, tp_i)
    sub, width = x_ref.shape
    block = sub * tp_n
    span = width // stops
    feats = span // 2
    units = gw_ref.shape[1]
    own_units = units // 2
    chunks = own_units // WIDTH
    items = groups * chunks
    cols = d_buf.shape[2]
    rs_depth = RS_LAG * (stops - 1)
    depth = rs_depth + AG_LAG * (stops - 1)
    bf16, f32 = jnp.bfloat16, jnp.float32

    my_h = jnp.where(seq_i < groups, 1, 0)
    my_g = jnp.where(seq_i < groups, seq_i, seq_n - 1 - seq_i)
    my_slot = my_g * 2 + my_h

    def block_of(g, h):
        return seq_n - 1 - g if h == 0 else g

    def before(h):
        return stops - 1 - pos if h == 0 else pos

    def step_of(h):
        return -1 if h == 0 else 1

    def at_stop(stop):
        return (stop * 2 + core, tp_i)

    def peer(j):
        return (tp_i + j) % tp_n

    def x_rows(slot, p):
        return pl.ds(pl.multiple_of(slot * block + p * sub, sub), sub)

    def remote(src, dst, snd, rcv, dev):
        return pltpu.make_async_remote_copy(
            src_ref=src, dst_ref=dst, send_sem=snd, recv_sem=rcv, device_id=dev, device_id_type=MESH)

    k_rows = pl.ds(pl.multiple_of(core * feats, feats), feats)
    up_gate = (gw_ref, uw_ref)

    def w_cols(q, c):
        return pl.ds(pl.multiple_of(q * own_units + c * WIDTH, WIDTH), WIDTH)

    def w_local(c, m):
        return pltpu.make_async_copy(
            up_gate[m].at[:, w_cols(core, c)], w_buf.at[c, k_rows, pl.ds(m * WIDTH, WIDTH)], w_sem.at[c, m])

    def w_push(c, m):
        return remote(
            up_gate[m].at[:, w_cols(1 - core, c)], w_buf.at[c, k_rows, pl.ds(m * WIDTH, WIDTH)],
            w_snd.at[c, m], w_rcv.at[c, m], partner)

    def w_land(c, m):
        there = pl.ds(pl.multiple_of((1 - core) * feats, feats), feats)
        return remote(
            up_gate[m].at[:, w_cols(core, c)], w_buf.at[c, there, pl.ds(m * WIDTH, WIDTH)],
            w_snd.at[c, m], w_rcv.at[c, m], partner)

    def d_copy(q):
        return pltpu.make_async_copy(dw_ref.at[q], d_buf.at[:, pl.ds(q * WIDTH, WIDTH)], d_sem.at[q])

    @pl.loop(0, chunks)
    def _(c):
        for m in range(2):
            w_local(c, m).start()

    barrier = pltpu.get_barrier_semaphore()
    for i in range(1, seq_n):
        pl.semaphore_signal(barrier, inc=1, device_id=((seq_i + i) % seq_n, tp_i), device_id_type=MESH)
    for j in range(1, tp_n):
        pl.semaphore_signal(barrier, inc=1, device_id=(seq_i, peer(j)), device_id_type=MESH)
    pl.semaphore_wait(barrier, seq_n + tp_n - 2)

    own_cols = pl.ds(pl.multiple_of(pos * span, span), span)

    def z_send(i):
        stop = (pos + i) % stops
        return remote(
            x_ref.at[:, pl.ds(pl.multiple_of(stop * span, span), span)], x_all.at[x_rows(my_slot, tp_i)],
            z_snd.at[i - 1], z_rcv.at[my_slot], at_stop(stop))

    def z_land(slot):
        return remote(
            x_ref.at[:, own_cols], x_all.at[x_rows(slot, tp_i)], z_snd.at[0], z_rcv.at[slot], at_stop((pos + 1) % stops))

    def t_send(src, slot, j):
        return remote(
            src, x_all.at[x_rows(slot, tp_i)], t_snd.at[slot, j - 1], t_rcv.at[slot, j - 1], (seq_i, peer(j)))

    def t_land(slot, j):
        rows = x_all.at[x_rows(slot, (tp_i + tp_n - j) % tp_n)]
        return remote(rows, rows, t_snd.at[slot, j - 1], t_rcv.at[slot, j - 1], (seq_i, peer(j)))

    def p_send(src, slot, p):
        return remote(src, x_all.at[x_rows(slot, p)], p_snd.at[slot, p], p_rcv.at[slot, p], partner)

    def p_land(slot, p):
        rows = x_all.at[x_rows(slot, p)]
        return remote(rows, rows, p_snd.at[slot, p], p_rcv.at[slot, p], partner)

    def source():
        for i in range(1, stops):
            z_send(i).start()
        mine = x_ref.at[:, own_cols]
        for j in range(1, tp_n):
            t_send(mine, my_slot, j).start()
        p_send(mine, my_slot, tp_i).start()

    def x_stage_a(g, h):
        b = block_of(g, h)
        slot = g * 2 + h

        @pl.when(jnp.logical_and(b % 2 == core, b // 2 != pos))
        def _():
            z_land(slot).wait_recv()
            mine = x_all.at[x_rows(slot, tp_i)]
            for j in range(1, tp_n):
                t_send(mine, slot, j).start()
            p_send(mine, slot, tp_i).start()

    def x_stage_b(g, h):
        b = block_of(g, h)
        slot = g * 2 + h

        @pl.when(b % 2 == core)
        def _():
            for j in range(1, tp_n):
                t_land(slot, j).wait_recv()
                p = (tp_i + tp_n - j) % tp_n
                p_send(x_all.at[x_rows(slot, p)], slot, p).start()

    def x_stage_c(g, h):
        b = block_of(g, h)
        slot = g * 2 + h

        @pl.when(b % 2 != core)
        def _():
            for p in range(tp_n):
                p_land(slot, p).wait_recv()

    def chain_copy(i, h):
        return remote(chain.at[h, i], chain.at[h, i], c_snd.at[h], c_rcv.at[h, i], at_stop(pos + step_of(h)))

    def back_copy(i, h):
        return remote(hid.at[h, i, core], hid.at[h, i, core], h_snd.at[h], h_rcv.at[h, i], at_stop(pos - step_of(h)))

    def side_copy(i, h):
        return remote(hid.at[h, i, core], hid.at[h, i, core], q_snd.at[h], q_rcv.at[h, i], partner)

    def side_land(i, h):
        return remote(hid.at[h, i, 1 - core], hid.at[h, i, 1 - core], q_snd.at[h], q_rcv.at[h, i], partner)

    def inside(i):
        return jnp.logical_and(i >= 0, i < items)

    def multiply(i, h):
        g, c = i // chunks, i % chunks
        rows = pl.ds(pl.multiple_of((g * 2 + h) * block, block), block)
        part[h] = jnp.dot(x_all[rows, :], w_buf[c], preferred_element_type=f32)

    def reduce(i, h):
        done = before(h)

        @pl.when(done == 0)
        def _():
            chain[h, i] = part[h].astype(bf16)

        @pl.when(done > 0)
        def _():
            chain_copy(i, h).wait_recv()

        @pl.when(jnp.logical_and(done > 0, done < stops - 1))
        def _():
            chain[h, i] = (part[h] + chain[h, i].astype(f32)).astype(bf16)

        @pl.when(done < stops - 1)
        def _():
            chain_copy(i, h).start()

        @pl.when(done == stops - 1)
        def _():
            both = part[h] + chain[h, i].astype(f32)
            gate = both[:, :WIDTH]
            hid[h, i, core] = (gate / (1.0 + jnp.exp(-gate)) * both[:, WIDTH:]).astype(bf16)
            back_copy(i, h).start()
            side_copy(i, h).start()

    def relay(i, h):
        done = before(h)

        @pl.when(done < stops - 1)
        def _():
            back_copy(i, h).wait_recv()

            @pl.when(done > 0)
            def _():
                back_copy(i, h).start()

            side_copy(i, h).start()

    def down(i):
        for h in range(2):
            side_land(i, h).wait_recv()
        c = i % chunks
        lhs = jnp.concatenate(
            [jnp.concatenate([hid[h, i, 0], hid[h, i, 1]], axis=1) for h in range(2)], axis=0)
        tile = min(cols, 2 * WIDTH)
        for n in range(0, cols, tile):
            acc[:, n : n + tile] += jnp.dot(lhs, d_buf[c, :, n : n + tile], preferred_element_type=f32)

    def tp_rows(h, p):
        return pl.ds(pl.multiple_of(h * block + p * sub, sub), sub)

    def s_copy(g, j, h):
        return remote(
            stage.at[g, tp_rows(h, peer(j))], got.at[g, j - 1, h], s_snd.at[g, j - 1, h], s_rcv.at[g, j - 1, h],
            (seq_i, peer(j)))

    my_cols = pl.ds(pl.multiple_of(seq_i * cols, cols), cols)

    def f_copy(g, h):
        return remote(
            fin.at[g, h], rows_out.at[:, my_cols], f_snd.at[g, h], f_rcv.at[seq_i], (block_of(g, h), tp_i))

    def f_land(origin):
        there = pl.ds(pl.multiple_of(origin * cols, cols), cols)
        return remote(fin.at[0, 0], rows_out.at[:, there], f_snd.at[0, 0], f_rcv.at[origin], (origin, tp_i))

    def spread(g):
        stage[g] = acc[...].astype(bf16)
        acc[...] = jnp.zeros_like(acc)
        for j in range(1, tp_n):
            for h in range(2):
                s_copy(g, j, h).start()

    def collect(g):
        for h in range(2):
            total = stage[g, tp_rows(h, tp_i), :].astype(f32)
            for j in range(1, tp_n):
                s_copy(g, j, h).wait_recv()
                total = total + got[g, j - 1, h].astype(f32)
            fin[g, h] = total.astype(bf16)

            @pl.when(block_of(g, h) != seq_i)
            def _():
                f_copy(g, h).start()

            @pl.when(block_of(g, h) == seq_i)
            def _():
                rows_out[:, my_cols] = fin[g, h]

    @pl.loop(0, chunks)
    def _(c):
        for m in range(2):
            w_push(c, m).start()

    for q in range(2):
        d_copy(q).start()
    x_all[x_rows(my_slot, tp_i), :] = x_ref[:, own_cols]
    acc[...] = jnp.zeros_like(acc)
    first_use = RS_LAG * jnp.minimum(before(0), before(1))
    source_step = jnp.maximum(my_g * chunks - SOURCE_LEAD, -RELAY_LEAD)

    def group_starts(s):
        return jnp.logical_and(jnp.logical_and(s >= 0, s < items), s % chunks == 0)

    @pl.loop(0, RELAY_LEAD + items + depth + 2 + OUT_LAG)
    def _(step):
        t = step - RELAY_LEAD
        i_rs = [t - RS_LAG * before(h) for h in range(2)]
        i_ag = [t - rs_depth - AG_LAG * (stops - 1 - before(h)) for h in range(2)]
        i_dn = t - depth - 1

        @pl.when(t == source_step)
        def _():
            source()

        for h in range(2):
            s = i_rs[h] + RELAY_LEAD

            @pl.when(group_starts(s))
            def _():
                x_stage_a(s // chunks, h)

        for h in range(2):
            s = i_rs[h] + PARTNER_LEAD

            @pl.when(group_starts(s))
            def _():
                x_stage_b(s // chunks, h)

        @pl.when(jnp.logical_and(t >= first_use, t < first_use + chunks))
        def _():
            c = t - first_use
            for m in range(2):
                w_local(c, m).wait()
                w_land(c, m).wait_recv()

        for h in range(2):
            @pl.when(inside(i_rs[h]))
            def _():
                @pl.when(i_rs[h] % chunks == 0)
                def _():
                    x_stage_c(i_rs[h] // chunks, h)

                multiply(i_rs[h], h)

        for h in range(2):
            @pl.when(inside(i_rs[h]))
            def _():
                reduce(i_rs[h], h)

        for h in range(2):
            @pl.when(inside(i_ag[h]))
            def _():
                relay(i_ag[h], h)

        @pl.when(i_dn == 0)
        def _():
            for q in range(2):
                d_copy(q).wait()

        @pl.when(inside(i_dn))
        def _():
            down(i_dn)

            @pl.when(i_dn % chunks == chunks - 1)
            def _():
                spread(i_dn // chunks)

        i_out = i_dn - OUT_LAG

        @pl.when(jnp.logical_and(inside(i_out), i_out % chunks == chunks - 1))
        def _():
            collect(i_out // chunks)

    for i in range(1, seq_n):
        f_land((seq_i + i) % seq_n).wait_recv()
    out_ref[...] = rows_out[...]

    for i in range(1, stops):
        z_send(i).wait_send()

    @pl.loop(0, chunks)
    def _(c):
        for m in range(2):
            w_push(c, m).wait_send()

    @pl.loop(0, groups)
    def _(g):
        for h in range(2):
            slot = g * 2 + h

            @pl.when(block_of(g, h) % 2 == core)
            def _():
                for j in range(1, tp_n):
                    t_land(slot, j).wait_send()
                for p in range(tp_n):
                    p_land(slot, p).wait_send()

            @pl.when(block_of(g, h) != seq_i)
            def _():
                f_copy(g, h).wait_send()

            for j in range(1, tp_n):
                s_copy(g, j, h).wait_send()

    for h in range(2):
        done = before(h)
        remote(hid.at[h, :, core], hid.at[h, :, core], q_snd.at[h], q_rcv.at[h, 0], partner).wait_send()

        @pl.when(done < stops - 1)
        def _():
            remote(chain.at[h], chain.at[h], c_snd.at[h], c_rcv.at[h, 0], partner).wait_send()

        @pl.when(done > 0)
        def _():
            remote(hid.at[h, :, core], hid.at[h, :, core], h_snd.at[h], h_rcv.at[h, 0], partner).wait_send()


def ffn(normed, gate_weight, up_weight, down_weight):
    seq_n, tp_n = lax.axis_size("seq"), lax.axis_size("tp")
    sub, width = normed.shape
    feats, units = gate_weight.shape
    cols = down_weight.shape[1]
    stops = groups = seq_n // 2
    block = sub * tp_n
    chunks = units // (2 * WIDTH)
    n = groups * chunks
    slots = 2 * groups
    bf16, f32 = jnp.bfloat16, jnp.float32
    dma = pltpu.SemaphoreType.DMA
    vmem = pl.BlockSpec(memory_space=pltpu.VMEM)
    anywhere = pl.BlockSpec(memory_space=pl.ANY)
    return pl.pallas_call(
        functools.partial(ffn_kernel, seq_n, tp_n),
        out_shape=jax.ShapeDtypeStruct((sub, seq_n * cols), bf16),
        in_specs=[vmem, anywhere, anywhere, anywhere],
        out_specs=vmem,
        scratch_shapes=[
            pltpu.VMEM((slots * block, 2 * feats), bf16),
            pltpu.VMEM((chunks, 2 * feats, 2 * WIDTH), bf16),
            pltpu.VMEM((chunks, 2 * WIDTH, cols), bf16),
            pltpu.VMEM((2, n, block, 2 * WIDTH), bf16),
            pltpu.VMEM((2, n, 2, block, WIDTH), bf16),
            pltpu.VMEM((2, block, 2 * WIDTH), f32),
            pltpu.VMEM((2 * block, cols), f32),
            pltpu.VMEM((groups, 2 * block, cols), bf16),
            pltpu.VMEM((groups, tp_n - 1, 2, sub, cols), bf16),
            pltpu.VMEM((groups, 2, sub, cols), bf16),
            pltpu.VMEM((sub, seq_n * cols), bf16),
            dma((chunks, 2)), dma((chunks, 2)), dma((chunks, 2)), dma((2,)),
            dma((stops - 1,)), dma((slots,)), dma((slots, tp_n - 1)), dma((slots, tp_n - 1)),
            dma((slots, tp_n)), dma((slots, tp_n)),
            dma((2,)), dma((2, n)), dma((2,)), dma((2, n)), dma((2,)), dma((2, n)),
            dma((groups, tp_n - 1, 2)), dma((groups, tp_n - 1, 2)), dma((groups, 2)), dma((seq_n,)),
        ],
        compiler_params=pltpu.CompilerParams(
            collective_id=0, has_side_effects=True, vmem_limit_bytes=63 * 1024 * 1024),
        cost_estimate=pl.CostEstimate(
            flops=6 * slots * block * feats * units, bytes_accessed=6 * feats * units, transcendentals=0),
    )(normed, gate_weight, up_weight, down_weight.reshape(2, chunks, WIDTH, cols))


def shards(tokens, conv_weight, norm_gain, gate_weight, up_weight, down_weight):
    tok_rows = tokens.shape[0]
    taps_count = conv_weight.shape[0]
    tp_count = lax.axis_size("tp")
    part_rows = tok_rows // tp_count
    edge_rows = from_behind(tokens[tok_rows - (taps_count - 1) :], "seq", 1)
    extended = jnp.concatenate([edge_rows, tokens], 0)
    extended = lax.dynamic_slice_in_dim(
        extended, lax.axis_index("tp") * part_rows, part_rows + taps_count - 1, 0).astype(jnp.float32)
    conv_out = jnp.zeros((part_rows, tokens.shape[1]), jnp.float32)
    for tap_index in range(taps_count):
        begin = taps_count - 1 - tap_index
        conv_out = conv_out + conv_weight[tap_index][None, :] * extended[begin : begin + part_rows]
    scale_rms = lax.rsqrt(jnp.mean(conv_out * conv_out, axis=-1, keepdims=True) + 1e-05)
    normed = (conv_out * scale_rms * norm_gain[None, :]).astype(jnp.bfloat16)
    return ffn(normed, gate_weight, up_weight, down_weight)


def solution(mesh):
    in_specs = (P("seq", None), P(), P(), P("seq", "tp"), P("seq", "tp"), P("tp", "seq"))
    out_specs = P(("seq", "tp"), None)
    return jax.shard_map(shards, mesh=mesh, in_specs=in_specs, out_specs=out_specs, check_vma=False)
```

```python
import functools

import jax
import jax.numpy as jnp
from jax import lax
from jax.experimental import pallas as pl
from jax.experimental.pallas import tpu as pltpu
from jax.sharding import PartitionSpec as P

MESH = pl.DeviceIdType.MESH
WIDTH = 128
RS_LAG = 3
AG_LAG = 3
SOURCE_LEAD = 10
RELAY_LEAD = 4
STAGGER = 2
EDGE = 16
CONV_TILE = 1024
PARTNER_LEAD = 1
OUT_LAG = 3


def ffn_kernel(seq_n, tp_n, taps_ref, gain_ref, tok_ref, gw_ref, uw_ref, dw_ref, out_ref,
               tok, edge, conv, x_ref, x_all, w_buf, d_buf, chain, hid, part, acc, stage, got, fin,
               tok_sem, edge_sem, e_snd, e_rcv, o_sem, w_sem, w_snd, w_rcv, d_sem, z_snd, z_rcv, t_snd, t_rcv, p_snd, p_rcv,
               c_snd, c_rcv, h_snd, h_rcv, q_snd, q_rcv, s_snd, s_rcv, f_snd, f_rcv):
    stops = seq_n // 2
    groups = seq_n // 2
    seq_i = lax.axis_index("seq")
    tp_i = lax.axis_index("tp")
    pos = seq_i // 2
    core = seq_i % 2
    partner = (pos * 2 + 1 - core, tp_i)
    sub, width = x_ref.shape
    block = sub * tp_n
    span = width // stops
    feats = span // 2
    units = gw_ref.shape[1]
    own_units = units // 2
    chunks = own_units // WIDTH
    items = groups * chunks
    cols = d_buf.shape[2]
    rs_depth = RS_LAG * (stops - 1)
    depth = rs_depth + AG_LAG * (stops - 1)
    bf16, f32 = jnp.bfloat16, jnp.float32

    my_h = jnp.where(seq_i < groups, 1, 0)
    my_g = jnp.where(seq_i < groups, seq_i, seq_n - 1 - seq_i)
    my_slot = my_g * 2 + my_h

    def block_of(g, h):
        return seq_n - 1 - g if h == 0 else g

    def before(h):
        return stops - 1 - pos if h == 0 else pos

    def step_of(h):
        return -1 if h == 0 else 1

    def at_stop(stop):
        return (stop * 2 + core, tp_i)

    def peer(j):
        return (tp_i + j) % tp_n

    def x_rows(slot, p):
        return pl.ds(pl.multiple_of(slot * block + p * sub, sub), sub)

    def remote(src, dst, snd, rcv, dev):
        return pltpu.make_async_remote_copy(
            src_ref=src, dst_ref=dst, send_sem=snd, recv_sem=rcv, device_id=dev, device_id_type=MESH)

    k_rows = pl.ds(pl.multiple_of(core * feats, feats), feats)
    up_gate = (gw_ref, uw_ref)

    def w_cols(q, c):
        return pl.ds(pl.multiple_of(q * own_units + c * WIDTH, WIDTH), WIDTH)

    def w_local(c, m):
        return pltpu.make_async_copy(
            up_gate[m].at[:, w_cols(core, c)], w_buf.at[c, k_rows, pl.ds(m * WIDTH, WIDTH)], w_sem.at[c, m])

    def w_push(c, m):
        return remote(
            up_gate[m].at[:, w_cols(1 - core, c)], w_buf.at[c, k_rows, pl.ds(m * WIDTH, WIDTH)],
            w_snd.at[c, m], w_rcv.at[c, m], partner)

    def w_land(c, m):
        there = pl.ds(pl.multiple_of((1 - core) * feats, feats), feats)
        return remote(
            up_gate[m].at[:, w_cols(core, c)], w_buf.at[c, there, pl.ds(m * WIDTH, WIDTH)],
            w_snd.at[c, m], w_rcv.at[c, m], partner)

    def d_copy(q):
        return pltpu.make_async_copy(dw_ref.at[q], d_buf.at[:, pl.ds(q * WIDTH, WIDTH)], d_sem.at[q])

    head = tp_i == 0
    body = pltpu.make_async_copy(
        tok_ref.at[pl.ds(0, sub)], tok.at[pl.ds(EDGE, sub)], tok_sem)
    with_edge = pltpu.make_async_copy(
        tok_ref.at[pl.ds(pl.multiple_of(jnp.maximum(tp_i * sub - EDGE, 0), EDGE), EDGE + sub)], tok, tok_sem)
    tail = pltpu.make_async_copy(tok_ref.at[pl.ds(block - EDGE, EDGE)], edge, edge_sem)
    edge_copy = remote(edge, tok.at[pl.ds(0, EDGE)], e_snd, e_rcv, ((seq_i + 1) % seq_n, tp_i))

    @pl.when(head)
    def _():
        body.start()
        tail.start()

    @pl.when(jnp.logical_not(head))
    def _():
        with_edge.start()

    @pl.loop(0, chunks)
    def _(c):
        for m in range(2):
            w_local(c, m).start()

    barrier = pltpu.get_barrier_semaphore()
    for i in range(1, seq_n):
        pl.semaphore_signal(barrier, inc=1, device_id=((seq_i + i) % seq_n, tp_i), device_id_type=MESH)
    for j in range(1, tp_n):
        pl.semaphore_signal(barrier, inc=1, device_id=(seq_i, peer(j)), device_id_type=MESH)

    def normalize():
        n_taps = taps_ref.shape[0]

        def convolve(n, squares):
            at = pl.ds(pl.multiple_of(n * CONV_TILE, CONV_TILE), CONV_TILE)
            rows = tok[:, at].astype(f32)
            total = jnp.zeros((sub, CONV_TILE), f32)
            for k in range(n_taps):
                moved = pltpu.roll(rows, k, 0) if k else rows
                total = total + taps_ref[k : k + 1, at] * moved[EDGE:]
            conv[:, at] = total
            return squares + jnp.sum(total * total, axis=1, keepdims=True)

        squares = lax.fori_loop(0, width // CONV_TILE, convolve, jnp.zeros((sub, 1), f32))
        scale = lax.rsqrt(squares / width + 1e-05)

        @pl.loop(0, width // CONV_TILE)
        def _(n):
            at = pl.ds(pl.multiple_of(n * CONV_TILE, CONV_TILE), CONV_TILE)
            x_ref[:, at] = (conv[:, at] * scale * gain_ref[:, at]).astype(bf16)

    @pl.when(jnp.logical_not(head))
    def _():
        with_edge.wait()
        normalize()

    pl.semaphore_wait(barrier, seq_n + tp_n - 2)

    @pl.when(head)
    def _():
        tail.wait()

        @pl.when(seq_i < seq_n - 1)
        def _():
            edge_copy.start()

        body.wait()

        @pl.when(seq_i == 0)
        def _():
            tok[0:EDGE, :] = jnp.zeros((EDGE, width), bf16)

        @pl.when(seq_i > 0)
        def _():
            edge_copy.wait_recv()

        normalize()

    own_cols = pl.ds(pl.multiple_of(pos * span, span), span)

    def z_stop(i):
        return (pos + jnp.where(my_h == 1, i, stops - i)) % stops

    def z_send(i):
        stop = z_stop(i)
        return remote(
            x_ref.at[:, pl.ds(pl.multiple_of(stop * span, span), span)], x_all.at[x_rows(my_slot, tp_i)],
            z_snd.at[i - 1], z_rcv.at[my_slot], at_stop(stop))

    def z_land(slot):
        return remote(
            x_ref.at[:, own_cols], x_all.at[x_rows(slot, tp_i)], z_snd.at[0], z_rcv.at[slot], at_stop((pos + 1) % stops))

    def t_send(src, slot, j):
        return remote(
            src, x_all.at[x_rows(slot, tp_i)], t_snd.at[slot, j - 1], t_rcv.at[slot, j - 1], (seq_i, peer(j)))

    def t_land(slot, j):
        rows = x_all.at[x_rows(slot, (tp_i + tp_n - j) % tp_n)]
        return remote(rows, rows, t_snd.at[slot, j - 1], t_rcv.at[slot, j - 1], (seq_i, peer(j)))

    def p_send(src, slot, p):
        return remote(src, x_all.at[x_rows(slot, p)], p_snd.at[slot, p], p_rcv.at[slot, p], partner)

    def p_land(slot, p):
        rows = x_all.at[x_rows(slot, p)]
        return remote(rows, rows, p_snd.at[slot, p], p_rcv.at[slot, p], partner)

    def source_far():
        for i in range(1, stops):
            z_send(i).start()

    def source():
        mine = x_ref.at[:, own_cols]
        for j in range(1, tp_n):
            t_send(mine, my_slot, j).start()
        p_send(mine, my_slot, tp_i).start()

    def x_stage_a(g, h):
        b = block_of(g, h)
        slot = g * 2 + h

        @pl.when(jnp.logical_and(b % 2 == core, b // 2 != pos))
        def _():
            z_land(slot).wait_recv()
            mine = x_all.at[x_rows(slot, tp_i)]
            for j in range(1, tp_n):
                t_send(mine, slot, j).start()
            p_send(mine, slot, tp_i).start()

    def x_stage_b(g, h):
        b = block_of(g, h)
        slot = g * 2 + h

        @pl.when(b % 2 == core)
        def _():
            for j in range(1, tp_n):
                t_land(slot, j).wait_recv()
                p = (tp_i + tp_n - j) % tp_n
                p_send(x_all.at[x_rows(slot, p)], slot, p).start()

    def x_stage_c(g, h):
        b = block_of(g, h)
        slot = g * 2 + h

        @pl.when(b % 2 != core)
        def _():
            for p in range(tp_n):
                p_land(slot, p).wait_recv()

    def chain_copy(i, h):
        return remote(chain.at[h, i], chain.at[h, i], c_snd.at[h], c_rcv.at[h, i], at_stop(pos + step_of(h)))

    def back_copy(i, h):
        return remote(hid.at[h, i, core], hid.at[h, i, core], h_snd.at[h], h_rcv.at[h, i], at_stop(pos - step_of(h)))

    def side_copy(i, h):
        return remote(hid.at[h, i, core], hid.at[h, i, core], q_snd.at[h], q_rcv.at[h, i], partner)

    def side_land(i, h):
        return remote(hid.at[h, i, 1 - core], hid.at[h, i, 1 - core], q_snd.at[h], q_rcv.at[h, i], partner)

    def inside(i):
        return jnp.logical_and(i >= 0, i < items)

    def multiply(i, h):
        g, c = i // chunks, i % chunks
        rows = pl.ds(pl.multiple_of((g * 2 + h) * block, block), block)
        part[h] = jnp.dot(x_all[rows, :], w_buf[c], preferred_element_type=f32)

    def reduce(i, h):
        done = before(h)

        @pl.when(done == 0)
        def _():
            chain[h, i] = part[h].astype(bf16)

        @pl.when(done > 0)
        def _():
            chain_copy(i, h).wait_recv()

        @pl.when(jnp.logical_and(done > 0, done < stops - 1))
        def _():
            chain[h, i] = (part[h] + chain[h, i].astype(f32)).astype(bf16)

        @pl.when(done < stops - 1)
        def _():
            chain_copy(i, h).start()

        @pl.when(done == stops - 1)
        def _():
            both = part[h] + chain[h, i].astype(f32)
            gate = both[:, :WIDTH]
            hid[h, i, core] = (gate / (1.0 + jnp.exp(-gate)) * both[:, WIDTH:]).astype(bf16)
            back_copy(i, h).start()
            side_copy(i, h).start()

    def relay(i, h):
        done = before(h)

        @pl.when(done < stops - 1)
        def _():
            back_copy(i, h).wait_recv()

            @pl.when(done > 0)
            def _():
                back_copy(i, h).start()

            side_copy(i, h).start()

    def down(i, h):
        side_land(i, h).wait_recv()
        c = i % chunks
        lhs = jnp.concatenate([hid[h, i, 0], hid[h, i, 1]], axis=1)
        tile = min(cols, 2 * WIDTH)
        for n in range(0, cols, tile):
            acc[h, :, n : n + tile] += jnp.dot(lhs, d_buf[c, :, n : n + tile], preferred_element_type=f32)

    def tp_rows(p):
        return pl.ds(pl.multiple_of(p * sub, sub), sub)

    def s_copy(g, j, h):
        return remote(
            stage.at[g, h, tp_rows(peer(j))], got.at[g, h, j - 1], s_snd.at[g, h, j - 1], s_rcv.at[g, h, j - 1],
            (seq_i, peer(j)))

    def f_copy(g, h):
        return remote(
            fin.at[g, h], out_ref.at[seq_i], f_snd.at[g, h], f_rcv.at[seq_i], (block_of(g, h), tp_i))

    def f_land(origin):
        return remote(fin.at[0, 0], out_ref.at[origin], f_snd.at[0, 0], f_rcv.at[origin], (origin, tp_i))

    keep = pltpu.make_async_copy(fin.at[my_g, my_h], out_ref.at[seq_i], o_sem)

    def spread(g, h):
        stage[g, h] = acc[h].astype(bf16)
        acc[h] = jnp.zeros_like(acc[h])
        for j in range(1, tp_n):
            s_copy(g, j, h).start()

    def collect(g, h):
        total = stage[g, h, tp_rows(tp_i), :].astype(f32)
        for j in range(1, tp_n):
            s_copy(g, j, h).wait_recv()
            total = total + got[g, h, j - 1].astype(f32)
        fin[g, h] = total.astype(bf16)

        @pl.when(block_of(g, h) != seq_i)
        def _():
            f_copy(g, h).start()

        @pl.when(block_of(g, h) == seq_i)
        def _():
            keep.start()

    @pl.loop(0, chunks)
    def _(c):
        for m in range(2):
            w_push(c, m).start()

    for q in range(2):
        d_copy(q).start()
    x_all[x_rows(my_slot, tp_i), :] = x_ref[:, own_cols]
    acc[...] = jnp.zeros_like(acc)
    first_use = RS_LAG * jnp.minimum(before(0), before(1))
    far_step = my_g * STAGGER - RELAY_LEAD
    source_step = jnp.maximum(my_g * chunks - SOURCE_LEAD, -RELAY_LEAD)

    def group_starts(s):
        return jnp.logical_and(jnp.logical_and(s >= 0, s < items), s % chunks == 0)

    @pl.loop(0, RELAY_LEAD + items + depth + 2 + OUT_LAG)
    def _(step):
        t = step - RELAY_LEAD
        i_rs = [t - RS_LAG * before(h) for h in range(2)]
        i_ag = [t - rs_depth - AG_LAG * (stops - 1 - before(h)) for h in range(2)]
        i_dn = [i - 1 for i in i_ag]
        i_out = [i - OUT_LAG for i in i_dn]

        @pl.when(t == source_step)
        def _():
            source()

        @pl.when(t == far_step)
        def _():
            source_far()

        for h in range(2):
            s = i_rs[h] + RELAY_LEAD

            @pl.when(group_starts(s))
            def _():
                x_stage_a(s // chunks, h)

        for h in range(2):
            s = i_rs[h] + PARTNER_LEAD

            @pl.when(group_starts(s))
            def _():
                x_stage_b(s // chunks, h)

        @pl.when(jnp.logical_and(t >= first_use, t < first_use + chunks))
        def _():
            c = t - first_use
            for m in range(2):
                w_local(c, m).wait()
                w_land(c, m).wait_recv()

        for h in range(2):
            @pl.when(inside(i_rs[h]))
            def _():
                @pl.when(i_rs[h] % chunks == 0)
                def _():
                    x_stage_c(i_rs[h] // chunks, h)

                multiply(i_rs[h], h)

        for h in range(2):
            @pl.when(inside(i_rs[h]))
            def _():
                reduce(i_rs[h], h)

        for h in range(2):
            @pl.when(inside(i_ag[h]))
            def _():
                relay(i_ag[h], h)

        @pl.when(t == rs_depth + 1)
        def _():
            for q in range(2):
                d_copy(q).wait()

        for h in range(2):
            @pl.when(inside(i_dn[h]))
            def _():
                down(i_dn[h], h)

                @pl.when(i_dn[h] % chunks == chunks - 1)
                def _():
                    spread(i_dn[h] // chunks, h)

            @pl.when(jnp.logical_and(inside(i_out[h]), i_out[h] % chunks == chunks - 1))
            def _():
                collect(i_out[h] // chunks, h)

    for i in range(1, seq_n):
        f_land((seq_i + i) % seq_n).wait_recv()
    keep.wait()

    @pl.when(jnp.logical_and(head, seq_i < seq_n - 1))
    def _():
        edge_copy.wait_send()

    for i in range(1, stops):
        z_send(i).wait_send()

    @pl.loop(0, chunks)
    def _(c):
        for m in range(2):
            w_push(c, m).wait_send()

    @pl.loop(0, groups)
    def _(g):
        for h in range(2):
            slot = g * 2 + h

            @pl.when(block_of(g, h) % 2 == core)
            def _():
                for j in range(1, tp_n):
                    t_land(slot, j).wait_send()
                for p in range(tp_n):
                    p_land(slot, p).wait_send()

            @pl.when(block_of(g, h) != seq_i)
            def _():
                f_copy(g, h).wait_send()

            for j in range(1, tp_n):
                s_copy(g, j, h).wait_send()

    for h in range(2):
        done = before(h)
        remote(hid.at[h, :, core], hid.at[h, :, core], q_snd.at[h], q_rcv.at[h, 0], partner).wait_send()

        @pl.when(done < stops - 1)
        def _():
            remote(chain.at[h], chain.at[h], c_snd.at[h], c_rcv.at[h, 0], partner).wait_send()

        @pl.when(done > 0)
        def _():
            remote(hid.at[h, :, core], hid.at[h, :, core], h_snd.at[h], h_rcv.at[h, 0], partner).wait_send()


def shards(tokens, conv_weight, norm_gain, gate_weight, up_weight, down_weight):
    seq_n, tp_n = lax.axis_size("seq"), lax.axis_size("tp")
    block, width = tokens.shape
    sub = block // tp_n
    feats, units = gate_weight.shape
    cols = down_weight.shape[1]
    stops = groups = seq_n // 2
    chunks = units // (2 * WIDTH)
    n = groups * chunks
    slots = 2 * groups
    bf16, f32 = jnp.bfloat16, jnp.float32
    dma = pltpu.SemaphoreType.DMA
    vmem = pl.BlockSpec(memory_space=pltpu.VMEM)
    anywhere = pl.BlockSpec(memory_space=pl.ANY)
    pieces = pl.pallas_call(
        functools.partial(ffn_kernel, seq_n, tp_n),
        out_shape=jax.ShapeDtypeStruct((seq_n, sub, cols), bf16),
        in_specs=[vmem, vmem, anywhere, anywhere, anywhere, anywhere],
        out_specs=anywhere,
        scratch_shapes=[
            pltpu.VMEM((EDGE + sub, width), bf16),
            pltpu.VMEM((EDGE, width), bf16),
            pltpu.VMEM((sub, width), f32),
            pltpu.VMEM((sub, width), bf16),
            pltpu.VMEM((slots * block, 2 * feats), bf16),
            pltpu.VMEM((chunks, 2 * feats, 2 * WIDTH), bf16),
            pltpu.VMEM((chunks, 2 * WIDTH, cols), bf16),
            pltpu.VMEM((2, n, block, 2 * WIDTH), bf16),
            pltpu.VMEM((2, n, 2, block, WIDTH), bf16),
            pltpu.VMEM((2, block, 2 * WIDTH), f32),
            pltpu.VMEM((2, block, cols), f32),
            pltpu.VMEM((groups, 2, block, cols), bf16),
            pltpu.VMEM((groups, 2, tp_n - 1, sub, cols), bf16),
            pltpu.VMEM((groups, 2, sub, cols), bf16),
            dma(()), dma(()), dma(()), dma(()), dma(()),
            dma((chunks, 2)), dma((chunks, 2)), dma((chunks, 2)), dma((2,)),
            dma((stops - 1,)), dma((slots,)), dma((slots, tp_n - 1)), dma((slots, tp_n - 1)),
            dma((slots, tp_n)), dma((slots, tp_n)),
            dma((2,)), dma((2, n)), dma((2,)), dma((2, n)), dma((2,)), dma((2, n)),
            dma((groups, 2, tp_n - 1)), dma((groups, 2, tp_n - 1)), dma((groups, 2)), dma((seq_n,)),
        ],
        compiler_params=pltpu.CompilerParams(
            collective_id=0, has_side_effects=True, vmem_limit_bytes=63 * 1024 * 1024),
        cost_estimate=pl.CostEstimate(
            flops=6 * slots * block * feats * units, bytes_accessed=6 * feats * units, transcendentals=0),
    )(conv_weight, norm_gain.reshape(1, width), tokens, gate_weight, up_weight,
      down_weight.reshape(2, chunks, WIDTH, cols))
    return jnp.transpose(pieces, (1, 0, 2)).reshape(sub, seq_n * cols)


def solution(mesh):
    in_specs = (P("seq", None), P(), P(), P("seq", "tp"), P("seq", "tp"), P("tp", "seq"))
    out_specs = P(("seq", "tp"), None)
    return jax.shard_map(shards, mesh=mesh, in_specs=in_specs, out_specs=out_specs, check_vma=False)
```

```python
import functools

import jax
import jax.numpy as jnp
from jax import lax
from jax.experimental import pallas as pl
from jax.experimental.pallas import tpu as pltpu
from jax.sharding import PartitionSpec as P

MESH = pl.DeviceIdType.MESH
WIDTH = 128
RS_LAG = 3
AG_LAG = 3
SOURCE_LEAD = 10
RELAY_LEAD = 4
STAGGER = 1
EDGE = 16
CONV_TILE = 1024
PARTNER_LEAD = 1
OUT_LAG = 3
HELD = 3
HELD_LEAD = 1


def ffn_kernel(seq_n, tp_n, taps_ref, gain_ref, tok_ref, gw_ref, uw_ref, dw_ref, out_ref,
               tok, edge, conv, x_ref, x_all, w_buf, d_buf, chain, hid, part, acc, stage, got, fin,
               tok_sem, edge_sem, e_snd, e_rcv, o_sem, w_sem, w_snd, w_rcv, d_sem, z_snd, z_rcv, t_snd, t_rcv, p_snd, p_rcv,
               c_snd, c_rcv, h_snd, h_rcv, q_snd, q_rcv, s_snd, s_rcv, f_snd, f_rcv):
    stops = seq_n // 2
    groups = seq_n // 2
    seq_i = lax.axis_index("seq")
    tp_i = lax.axis_index("tp")
    pos = seq_i // 2
    core = seq_i % 2
    partner = (pos * 2 + 1 - core, tp_i)
    sub, width = x_ref.shape
    block = sub * tp_n
    span = width // stops
    feats = span // 2
    units = gw_ref.shape[1]
    own_units = units // 2
    chunks = own_units // WIDTH
    items = groups * chunks
    cols = d_buf.shape[2]
    rs_depth = RS_LAG * (stops - 1)
    depth = rs_depth + AG_LAG * (stops - 1)
    held = min(HELD, groups - 1)
    bf16, f32 = jnp.bfloat16, jnp.float32

    my_h = jnp.where(seq_i < groups, 1, 0)
    my_g = jnp.where(seq_i < groups, seq_i, seq_n - 1 - seq_i)
    my_slot = my_g * 2 + my_h

    def block_of(g, h):
        return seq_n - 1 - g if h == 0 else g

    def before(h):
        return stops - 1 - pos if h == 0 else pos

    def step_of(h):
        return -1 if h == 0 else 1

    def at_stop(stop):
        return (stop * 2 + core, tp_i)

    def peer(j):
        return (tp_i + j) % tp_n

    def x_rows(slot, p):
        return pl.ds(pl.multiple_of(slot * block + p * sub, sub), sub)

    def remote(src, dst, snd, rcv, dev):
        return pltpu.make_async_remote_copy(
            src_ref=src, dst_ref=dst, send_sem=snd, recv_sem=rcv, device_id=dev, device_id_type=MESH)

    k_rows = pl.ds(pl.multiple_of(core * feats, feats), feats)
    up_gate = (gw_ref, uw_ref)

    def w_cols(q, c):
        return pl.ds(pl.multiple_of(q * own_units + c * WIDTH, WIDTH), WIDTH)

    def w_local(c, m):
        return pltpu.make_async_copy(
            up_gate[m].at[:, w_cols(core, c)], w_buf.at[c, k_rows, pl.ds(m * WIDTH, WIDTH)], w_sem.at[c, m])

    def w_push(c, m):
        return remote(
            up_gate[m].at[:, w_cols(1 - core, c)], w_buf.at[c, k_rows, pl.ds(m * WIDTH, WIDTH)],
            w_snd.at[c, m], w_rcv.at[c, m], partner)

    def w_land(c, m):
        there = pl.ds(pl.multiple_of((1 - core) * feats, feats), feats)
        return remote(
            up_gate[m].at[:, w_cols(core, c)], w_buf.at[c, there, pl.ds(m * WIDTH, WIDTH)],
            w_snd.at[c, m], w_rcv.at[c, m], partner)

    def d_copy(q):
        return pltpu.make_async_copy(dw_ref.at[q], d_buf.at[:, pl.ds(q * WIDTH, WIDTH)], d_sem.at[q])

    head = tp_i == 0
    body = pltpu.make_async_copy(
        tok_ref.at[pl.ds(0, sub)], tok.at[pl.ds(EDGE, sub)], tok_sem)
    with_edge = pltpu.make_async_copy(
        tok_ref.at[pl.ds(pl.multiple_of(jnp.maximum(tp_i * sub - EDGE, 0), EDGE), EDGE + sub)], tok, tok_sem)
    tail = pltpu.make_async_copy(tok_ref.at[pl.ds(block - EDGE, EDGE)], edge, edge_sem)
    edge_copy = remote(edge, tok.at[pl.ds(0, EDGE)], e_snd, e_rcv, ((seq_i + 1) % seq_n, tp_i))

    @pl.when(head)
    def _():
        body.start()
        tail.start()

    @pl.when(jnp.logical_not(head))
    def _():
        with_edge.start()

    @pl.loop(0, chunks)
    def _(c):
        for m in range(2):
            w_local(c, m).start()

    barrier = pltpu.get_barrier_semaphore()
    for i in range(1, seq_n):
        pl.semaphore_signal(barrier, inc=1, device_id=((seq_i + i) % seq_n, tp_i), device_id_type=MESH)
    for j in range(1, tp_n):
        pl.semaphore_signal(barrier, inc=1, device_id=(seq_i, peer(j)), device_id_type=MESH)

    def normalize():
        n_taps = taps_ref.shape[0]

        def convolve(n, squares):
            at = pl.ds(pl.multiple_of(n * CONV_TILE, CONV_TILE), CONV_TILE)
            rows = tok[:, at].astype(f32)
            total = jnp.zeros((sub, CONV_TILE), f32)
            for k in range(n_taps):
                moved = pltpu.roll(rows, k, 0) if k else rows
                total = total + taps_ref[k : k + 1, at] * moved[EDGE:]
            conv[:, at] = total
            return squares + jnp.sum(total * total, axis=1, keepdims=True)

        squares = lax.fori_loop(0, width // CONV_TILE, convolve, jnp.zeros((sub, 1), f32))
        scale = lax.rsqrt(squares / width + 1e-05)

        @pl.loop(0, width // CONV_TILE)
        def _(n):
            at = pl.ds(pl.multiple_of(n * CONV_TILE, CONV_TILE), CONV_TILE)
            x_ref[:, at] = (conv[:, at] * scale * gain_ref[:, at]).astype(bf16)

    @pl.when(jnp.logical_not(head))
    def _():
        with_edge.wait()
        normalize()

    pl.semaphore_wait(barrier, seq_n + tp_n - 2)

    @pl.when(jnp.logical_and(head, seq_i < seq_n - 1))
    def _():
        tail.wait()
        edge_copy.start()

    @pl.when(jnp.logical_and(head, seq_i == seq_n - 1))
    def _():
        tail.wait()

    @pl.loop(0, chunks)
    def _(c):
        for m in range(2):
            w_push(c, m).start()

    for q in range(2):
        d_copy(q).start()

    def prepare():
        @pl.when(head)
        def _():
            body.wait()

            @pl.when(seq_i == 0)
            def _():
                tok[0:EDGE, :] = jnp.zeros((EDGE, width), bf16)

            @pl.when(seq_i > 0)
            def _():
                edge_copy.wait_recv()

            normalize()

        x_all[x_rows(my_slot, tp_i), :] = x_ref[:, own_cols]

    own_cols = pl.ds(pl.multiple_of(pos * span, span), span)

    def z_stop(i):
        return (pos + jnp.where(my_h == 1, i, stops - i)) % stops

    def z_send(i):
        stop = z_stop(i)
        return remote(
            x_ref.at[:, pl.ds(pl.multiple_of(stop * span, span), span)], x_all.at[x_rows(my_slot, tp_i)],
            z_snd.at[i - 1], z_rcv.at[my_slot], at_stop(stop))

    def z_land(slot):
        return remote(
            x_ref.at[:, own_cols], x_all.at[x_rows(slot, tp_i)], z_snd.at[0], z_rcv.at[slot], at_stop((pos + 1) % stops))

    def t_send(src, slot, j):
        return remote(
            src, x_all.at[x_rows(slot, tp_i)], t_snd.at[slot, j - 1], t_rcv.at[slot, j - 1], (seq_i, peer(j)))

    def t_land(slot, j):
        rows = x_all.at[x_rows(slot, (tp_i + tp_n - j) % tp_n)]
        return remote(rows, rows, t_snd.at[slot, j - 1], t_rcv.at[slot, j - 1], (seq_i, peer(j)))

    def p_send(src, slot, p):
        return remote(src, x_all.at[x_rows(slot, p)], p_snd.at[slot, p], p_rcv.at[slot, p], partner)

    def p_land(slot, p):
        rows = x_all.at[x_rows(slot, p)]
        return remote(rows, rows, p_snd.at[slot, p], p_rcv.at[slot, p], partner)

    def source_far():
        for i in range(1, stops):
            z_send(i).start()

    def source():
        mine = x_ref.at[:, own_cols]
        for j in range(1, tp_n):
            t_send(mine, my_slot, j).start()
        p_send(mine, my_slot, tp_i).start()

    def x_stage_a(g, h):
        b = block_of(g, h)
        slot = g * 2 + h

        @pl.when(jnp.logical_and(b % 2 == core, b // 2 != pos))
        def _():
            z_land(slot).wait_recv()
            mine = x_all.at[x_rows(slot, tp_i)]
            for j in range(1, tp_n):
                t_send(mine, slot, j).start()
            p_send(mine, slot, tp_i).start()

    def x_stage_b(g, h):
        b = block_of(g, h)
        slot = g * 2 + h

        @pl.when(b % 2 == core)
        def _():
            for j in range(1, tp_n):
                t_land(slot, j).wait_recv()
                p = (tp_i + tp_n - j) % tp_n
                p_send(x_all.at[x_rows(slot, p)], slot, p).start()

    def x_stage_c(g, h):
        b = block_of(g, h)
        slot = g * 2 + h

        @pl.when(b % 2 != core)
        def _():
            for p in range(tp_n):
                p_land(slot, p).wait_recv()

    def chain_copy(i, h):
        return remote(chain.at[h, i], chain.at[h, i], c_snd.at[h], c_rcv.at[h, i], at_stop(pos + step_of(h)))

    def back_copy(i, h):
        return remote(hid.at[h, i, core], hid.at[h, i, core], h_snd.at[h], h_rcv.at[h, i], at_stop(pos - step_of(h)))

    def side_copy(i, h):
        return remote(hid.at[h, i, core], hid.at[h, i, core], q_snd.at[h], q_rcv.at[h, i], partner)

    def side_land(i, h):
        return remote(hid.at[h, i, 1 - core], hid.at[h, i, 1 - core], q_snd.at[h], q_rcv.at[h, i], partner)

    def inside(i):
        return jnp.logical_and(i >= 0, i < items)

    def multiply(i, h):
        g, c = i // chunks, i % chunks
        rows = pl.ds(pl.multiple_of((g * 2 + h) * block, block), block)
        part[h] = jnp.dot(x_all[rows, :], w_buf[c], preferred_element_type=f32)

    def reduce(i, h):
        done = before(h)

        @pl.when(done == 0)
        def _():
            chain[h, i] = part[h].astype(bf16)

        @pl.when(done > 0)
        def _():
            chain_copy(i, h).wait_recv()

        @pl.when(jnp.logical_and(done > 0, done < stops - 1))
        def _():
            chain[h, i] = (part[h] + chain[h, i].astype(f32)).astype(bf16)

        @pl.when(done < stops - 1)
        def _():
            chain_copy(i, h).start()

        @pl.when(done == stops - 1)
        def _():
            both = part[h] + chain[h, i].astype(f32)
            gate = both[:, :WIDTH]
            hid[h, i, core] = (gate / (1.0 + jnp.exp(-gate)) * both[:, WIDTH:]).astype(bf16)
            back_copy(i, h).start()
            side_copy(i, h).start()

    def relay(i, h):
        done = before(h)

        @pl.when(done < stops - 1)
        def _():
            back_copy(i, h).wait_recv()

            @pl.when(done > 0)
            def _():
                back_copy(i, h).start()

            side_copy(i, h).start()

    def down(i, h):
        side_land(i, h).wait_recv()
        c = i % chunks
        lhs = jnp.concatenate([hid[h, i, 0], hid[h, i, 1]], axis=1)
        tile = min(cols, 2 * WIDTH)
        for n in range(0, cols, tile):
            acc[h, :, n : n + tile] += jnp.dot(lhs, d_buf[c, :, n : n + tile], preferred_element_type=f32)

    def tp_rows(p):
        return pl.ds(pl.multiple_of(p * sub, sub), sub)

    def s_copy(g, j, h):
        return remote(
            stage.at[g, h, tp_rows(peer(j))], got.at[g, h, j - 1], s_snd.at[g, h, j - 1], s_rcv.at[g, h, j - 1],
            (seq_i, peer(j)))

    def f_copy(g, h):
        return remote(
            fin.at[g, h], out_ref.at[seq_i], f_snd.at[g, h], f_rcv.at[seq_i], (block_of(g, h), tp_i))

    def f_land(origin):
        return remote(fin.at[0, 0], out_ref.at[origin], f_snd.at[0, 0], f_rcv.at[origin], (origin, tp_i))

    keep = pltpu.make_async_copy(fin.at[my_g, my_h], out_ref.at[seq_i], o_sem)

    def spread(g, h):
        stage[g, h] = acc[h].astype(bf16)
        acc[h] = jnp.zeros_like(acc[h])
        for j in range(1, tp_n):
            s_copy(g, j, h).start()

    def collect(g, h):
        total = stage[g, h, tp_rows(tp_i), :].astype(f32)
        for j in range(1, tp_n):
            s_copy(g, j, h).wait_recv()
            total = total + got[g, h, j - 1].astype(f32)
        fin[g, h] = total.astype(bf16)

        @pl.when(block_of(g, h) != seq_i)
        def _():
            f_copy(g, h).start()

        @pl.when(block_of(g, h) == seq_i)
        def _():
            keep.start()

    acc[...] = jnp.zeros_like(acc)
    first_use = RS_LAG * jnp.minimum(before(0), before(1))
    far_step = my_g * STAGGER - RELAY_LEAD
    source_step = jnp.maximum(my_g * chunks - SOURCE_LEAD, -RELAY_LEAD)
    prepare_step = jnp.minimum(far_step, source_step)

    def group_starts(s):
        return jnp.logical_and(jnp.logical_and(s >= 0, s < items), s % chunks == 0)

    @pl.loop(0, RELAY_LEAD + items + depth + 2 + OUT_LAG)
    def _(step):
        t = step - RELAY_LEAD
        i_rs = [t - RS_LAG * before(h) for h in range(2)]
        i_ag = [t - rs_depth - AG_LAG * (stops - 1 - before(h)) for h in range(2)]
        i_dn = [i - 1 for i in i_ag]
        i_out = [i - OUT_LAG for i in i_dn]

        @pl.when(t == prepare_step)
        def _():
            prepare()

        @pl.when(t == source_step)
        def _():
            source()

        @pl.when(t == far_step)
        def _():
            source_far()

        for h in range(2):
            s = i_rs[h] + RELAY_LEAD

            @pl.when(group_starts(s))
            def _():
                x_stage_a(s // chunks, h)

        for h in range(2):
            s = i_rs[h] + PARTNER_LEAD

            @pl.when(group_starts(s))
            def _():
                x_stage_b(s // chunks, h)

        @pl.when(jnp.logical_and(t >= first_use, t < first_use + chunks))
        def _():
            c = t - first_use
            for m in range(2):
                w_local(c, m).wait()
                w_land(c, m).wait_recv()

        for h in range(2):
            @pl.when(inside(i_rs[h]))
            def _():
                @pl.when(i_rs[h] % chunks == 0)
                def _():
                    x_stage_c(i_rs[h] // chunks, h)

                multiply(i_rs[h], h)

        for h in range(2):
            @pl.when(inside(i_rs[h]))
            def _():
                reduce(i_rs[h], h)

        for h in range(2):
            @pl.when(inside(i_ag[h]))
            def _():
                relay(i_ag[h], h)

        @pl.when(t == rs_depth + 1)
        def _():
            for q in range(2):
                d_copy(q).wait()

        for h in range(2):
            @pl.when(inside(i_dn[h]))
            def _():
                down(i_dn[h], h)

                @pl.when(i_dn[h] % chunks == chunks - 1)
                def _():
                    spread(i_dn[h] // chunks, h)

            g_out = i_out[h] // chunks
            in_turn = jnp.logical_or(g_out < groups - 1 - held, g_out == groups - 1)

            @pl.when(jnp.logical_and(jnp.logical_and(inside(i_out[h]), i_out[h] % chunks == chunks - 1), in_turn))
            def _():
                collect(g_out, h)

        if held:
            @pl.when(t == items + depth - HELD_LEAD)
            def _():
                for g in range(groups - 1 - held, groups - 1):
                    for h in range(2):
                        collect(g, h)

    for i in range(1, seq_n):
        f_land((seq_i + i) % seq_n).wait_recv()
    keep.wait()

    @pl.when(jnp.logical_and(head, seq_i < seq_n - 1))
    def _():
        edge_copy.wait_send()

    for i in range(1, stops):
        z_send(i).wait_send()

    @pl.loop(0, chunks)
    def _(c):
        for m in range(2):
            w_push(c, m).wait_send()

    @pl.loop(0, groups)
    def _(g):
        for h in range(2):
            slot = g * 2 + h

            @pl.when(block_of(g, h) % 2 == core)
            def _():
                for j in range(1, tp_n):
                    t_land(slot, j).wait_send()
                for p in range(tp_n):
                    p_land(slot, p).wait_send()

            @pl.when(block_of(g, h) != seq_i)
            def _():
                f_copy(g, h).wait_send()

            for j in range(1, tp_n):
                s_copy(g, j, h).wait_send()

    for h in range(2):
        done = before(h)
        remote(hid.at[h, :, core], hid.at[h, :, core], q_snd.at[h], q_rcv.at[h, 0], partner).wait_send()

        @pl.when(done < stops - 1)
        def _():
            remote(chain.at[h], chain.at[h], c_snd.at[h], c_rcv.at[h, 0], partner).wait_send()

        @pl.when(done > 0)
        def _():
            remote(hid.at[h, :, core], hid.at[h, :, core], h_snd.at[h], h_rcv.at[h, 0], partner).wait_send()


def shards(tokens, conv_weight, norm_gain, gate_weight, up_weight, down_weight):
    seq_n, tp_n = lax.axis_size("seq"), lax.axis_size("tp")
    block, width = tokens.shape
    sub = block // tp_n
    feats, units = gate_weight.shape
    cols = down_weight.shape[1]
    stops = groups = seq_n // 2
    chunks = units // (2 * WIDTH)
    n = groups * chunks
    slots = 2 * groups
    bf16, f32 = jnp.bfloat16, jnp.float32
    dma = pltpu.SemaphoreType.DMA
    vmem = pl.BlockSpec(memory_space=pltpu.VMEM)
    anywhere = pl.BlockSpec(memory_space=pl.ANY)
    pieces = pl.pallas_call(
        functools.partial(ffn_kernel, seq_n, tp_n),
        out_shape=jax.ShapeDtypeStruct((seq_n, sub, cols), bf16),
        in_specs=[vmem, vmem, anywhere, anywhere, anywhere, anywhere],
        out_specs=anywhere,
        scratch_shapes=[
            pltpu.VMEM((EDGE + sub, width), bf16),
            pltpu.VMEM((EDGE, width), bf16),
            pltpu.VMEM((sub, width), f32),
            pltpu.VMEM((sub, width), bf16),
            pltpu.VMEM((slots * block, 2 * feats), bf16),
            pltpu.VMEM((chunks, 2 * feats, 2 * WIDTH), bf16),
            pltpu.VMEM((chunks, 2 * WIDTH, cols), bf16),
            pltpu.VMEM((2, n, block, 2 * WIDTH), bf16),
            pltpu.VMEM((2, n, 2, block, WIDTH), bf16),
            pltpu.VMEM((2, block, 2 * WIDTH), f32),
            pltpu.VMEM((2, block, cols), f32),
            pltpu.VMEM((groups, 2, block, cols), bf16),
            pltpu.VMEM((groups, 2, tp_n - 1, sub, cols), bf16),
            pltpu.VMEM((groups, 2, sub, cols), bf16),
            dma(()), dma(()), dma(()), dma(()), dma(()),
            dma((chunks, 2)), dma((chunks, 2)), dma((chunks, 2)), dma((2,)),
            dma((stops - 1,)), dma((slots,)), dma((slots, tp_n - 1)), dma((slots, tp_n - 1)),
            dma((slots, tp_n)), dma((slots, tp_n)),
            dma((2,)), dma((2, n)), dma((2,)), dma((2, n)), dma((2,)), dma((2, n)),
            dma((groups, 2, tp_n - 1)), dma((groups, 2, tp_n - 1)), dma((groups, 2)), dma((seq_n,)),
        ],
        compiler_params=pltpu.CompilerParams(
            collective_id=0, has_side_effects=True, vmem_limit_bytes=63 * 1024 * 1024),
        cost_estimate=pl.CostEstimate(
            flops=6 * slots * block * feats * units, bytes_accessed=6 * feats * units, transcendentals=0),
    )(conv_weight, norm_gain.reshape(1, width), tokens, gate_weight, up_weight,
      down_weight.reshape(2, chunks, WIDTH, cols))
    return jnp.transpose(pieces, (1, 0, 2)).reshape(sub, seq_n * cols)


def solution(mesh):
    in_specs = (P("seq", None), P(), P(), P("seq", "tp"), P("seq", "tp"), P("tp", "seq"))
    out_specs = P(("seq", "tp"), None)
    return jax.shard_map(shards, mesh=mesh, in_specs=in_specs, out_specs=out_specs, check_vma=False)
```

```python
import functools

import jax
import jax.numpy as jnp
from jax import lax
from jax.experimental import pallas as pl
from jax.experimental.pallas import tpu as pltpu
from jax.sharding import PartitionSpec as P

MESH = pl.DeviceIdType.MESH
WIDTH = 128
RS_LAG = 3
AG_LAG = 3
SOURCE_LEAD = 10
RELAY_LEAD = 6
STAGGER = 1
EDGE = 16
CONV_TILE = 1024
PARTNER_LEAD = 1
OUT_LAG = 3
HELD = 3
HELD_LEAD = 1


def ffn_kernel(seq_n, tp_n, taps_hbm, gain_hbm, tok_ref, gw_ref, uw_ref, dw_ref, out_ref,
               taps_ref, gain_ref, tok, edge, conv, x_ref, x_all, w_buf, d_buf, chain, hid, part, acc, stage, got, fin,
               taps_sem, gain_sem, tok_sem, edge_sem, e_snd, e_rcv, o_sem, w_sem, w_snd, w_rcv, d_sem, z_snd, z_rcv, t_snd, t_rcv, p_snd, p_rcv,
               c_snd, c_rcv, h_snd, h_rcv, q_snd, q_rcv, s_snd, s_rcv, f_snd, f_rcv):
    stops = seq_n // 2
    groups = seq_n // 2
    seq_i = lax.axis_index("seq")
    tp_i = lax.axis_index("tp")
    pos = seq_i // 2
    core = seq_i % 2
    partner = (pos * 2 + 1 - core, tp_i)
    sub, width = x_ref.shape
    block = sub * tp_n
    span = width // stops
    feats = span // 2
    units = gw_ref.shape[1]
    own_units = units // 2
    chunks = own_units // WIDTH
    items = groups * chunks
    cols = d_buf.shape[2]
    rs_depth = RS_LAG * (stops - 1)
    depth = rs_depth + AG_LAG * (stops - 1)
    held = min(HELD, groups - 1)
    bf16, f32 = jnp.bfloat16, jnp.float32

    my_h = jnp.where(seq_i < groups, 1, 0)
    my_g = jnp.where(seq_i < groups, seq_i, seq_n - 1 - seq_i)
    my_slot = my_g * 2 + my_h

    def block_of(g, h):
        return seq_n - 1 - g if h == 0 else g

    def before(h):
        return stops - 1 - pos if h == 0 else pos

    def step_of(h):
        return -1 if h == 0 else 1

    def at_stop(stop):
        return (stop * 2 + core, tp_i)

    def peer(j):
        return (tp_i + j) % tp_n

    def x_rows(slot, p):
        return pl.ds(pl.multiple_of(slot * block + p * sub, sub), sub)

    def remote(src, dst, snd, rcv, dev):
        return pltpu.make_async_remote_copy(
            src_ref=src, dst_ref=dst, send_sem=snd, recv_sem=rcv, device_id=dev, device_id_type=MESH)

    k_rows = pl.ds(pl.multiple_of(core * feats, feats), feats)
    up_gate = (gw_ref, uw_ref)

    def w_cols(q, c):
        return pl.ds(pl.multiple_of(q * own_units + c * WIDTH, WIDTH), WIDTH)

    def w_local(c, m):
        return pltpu.make_async_copy(
            up_gate[m].at[:, w_cols(core, c)], w_buf.at[c, k_rows, pl.ds(m * WIDTH, WIDTH)], w_sem.at[c, m])

    def w_push(c, m):
        return remote(
            up_gate[m].at[:, w_cols(1 - core, c)], w_buf.at[c, k_rows, pl.ds(m * WIDTH, WIDTH)],
            w_snd.at[c, m], w_rcv.at[c, m], partner)

    def w_land(c, m):
        there = pl.ds(pl.multiple_of((1 - core) * feats, feats), feats)
        return remote(
            up_gate[m].at[:, w_cols(core, c)], w_buf.at[c, there, pl.ds(m * WIDTH, WIDTH)],
            w_snd.at[c, m], w_rcv.at[c, m], partner)

    def d_copy(q):
        return pltpu.make_async_copy(dw_ref.at[q], d_buf.at[:, pl.ds(q * WIDTH, WIDTH)], d_sem.at[q])

    taps_copy = pltpu.make_async_copy(taps_hbm, taps_ref, taps_sem)
    gain_copy = pltpu.make_async_copy(gain_hbm, gain_ref, gain_sem)
    taps_copy.start()
    gain_copy.start()
    head = tp_i == 0
    body = pltpu.make_async_copy(
        tok_ref.at[pl.ds(0, sub)], tok.at[pl.ds(EDGE, sub)], tok_sem)
    with_edge = pltpu.make_async_copy(
        tok_ref.at[pl.ds(pl.multiple_of(jnp.maximum(tp_i * sub - EDGE, 0), EDGE), EDGE + sub)], tok, tok_sem)
    tail = pltpu.make_async_copy(tok_ref.at[pl.ds(block - EDGE, EDGE)], edge, edge_sem)
    edge_copy = remote(edge, tok.at[pl.ds(0, EDGE)], e_snd, e_rcv, ((seq_i + 1) % seq_n, tp_i))

    @pl.when(head)
    def _():
        body.start()
        tail.start()

    @pl.when(jnp.logical_not(head))
    def _():
        with_edge.start()

    @pl.loop(0, chunks)
    def _(c):
        for m in range(2):
            w_local(c, m).start()

    barrier = pltpu.get_barrier_semaphore()
    for i in range(1, seq_n):
        pl.semaphore_signal(barrier, inc=1, device_id=((seq_i + i) % seq_n, tp_i), device_id_type=MESH)
    for j in range(1, tp_n):
        pl.semaphore_signal(barrier, inc=1, device_id=(seq_i, peer(j)), device_id_type=MESH)

    def normalize():
        taps_copy.wait()
        gain_copy.wait()
        n_taps = taps_ref.shape[0]

        def convolve(n, squares):
            at = pl.ds(pl.multiple_of(n * CONV_TILE, CONV_TILE), CONV_TILE)
            rows = tok[:, at].astype(f32)
            total = jnp.zeros((sub, CONV_TILE), f32)
            for k in range(n_taps):
                moved = pltpu.roll(rows, k, 0) if k else rows
                total = total + taps_ref[k : k + 1, at] * moved[EDGE:]
            conv[:, at] = total
            return squares + jnp.sum(total * total, axis=1, keepdims=True)

        squares = lax.fori_loop(0, width // CONV_TILE, convolve, jnp.zeros((sub, 1), f32))
        scale = lax.rsqrt(squares / width + 1e-05)

        @pl.loop(0, width // CONV_TILE)
        def _(n):
            at = pl.ds(pl.multiple_of(n * CONV_TILE, CONV_TILE), CONV_TILE)
            x_ref[:, at] = (conv[:, at] * scale * gain_ref[:, at]).astype(bf16)

    @pl.when(jnp.logical_not(head))
    def _():
        with_edge.wait()
        normalize()

    pl.semaphore_wait(barrier, seq_n + tp_n - 2)

    @pl.when(jnp.logical_and(head, seq_i < seq_n - 1))
    def _():
        tail.wait()
        edge_copy.start()

    @pl.when(jnp.logical_and(head, seq_i == seq_n - 1))
    def _():
        tail.wait()

    @pl.loop(0, chunks)
    def _(c):
        for m in range(2):
            w_push(c, m).start()

    for q in range(2):
        d_copy(q).start()

    def prepare():
        @pl.when(head)
        def _():
            body.wait()

            @pl.when(seq_i == 0)
            def _():
                tok[0:EDGE, :] = jnp.zeros((EDGE, width), bf16)

            @pl.when(seq_i > 0)
            def _():
                edge_copy.wait_recv()

            normalize()

        x_all[x_rows(my_slot, tp_i), :] = x_ref[:, own_cols]

    own_cols = pl.ds(pl.multiple_of(pos * span, span), span)

    def z_stop(i):
        return (pos + jnp.where(my_h == 1, i, stops - i)) % stops

    def z_send(i):
        stop = z_stop(i)
        return remote(
            x_ref.at[:, pl.ds(pl.multiple_of(stop * span, span), span)], x_all.at[x_rows(my_slot, tp_i)],
            z_snd.at[i - 1], z_rcv.at[my_slot], at_stop(stop))

    def z_land(slot):
        return remote(
            x_ref.at[:, own_cols], x_all.at[x_rows(slot, tp_i)], z_snd.at[0], z_rcv.at[slot], at_stop((pos + 1) % stops))

    def t_send(src, slot, j):
        return remote(
            src, x_all.at[x_rows(slot, tp_i)], t_snd.at[slot, j - 1], t_rcv.at[slot, j - 1], (seq_i, peer(j)))

    def t_land(slot, j):
        rows = x_all.at[x_rows(slot, (tp_i + tp_n - j) % tp_n)]
        return remote(rows, rows, t_snd.at[slot, j - 1], t_rcv.at[slot, j - 1], (seq_i, peer(j)))

    def p_send(src, slot, p):
        return remote(src, x_all.at[x_rows(slot, p)], p_snd.at[slot, p], p_rcv.at[slot, p], partner)

    def p_land(slot, p):
        rows = x_all.at[x_rows(slot, p)]
        return remote(rows, rows, p_snd.at[slot, p], p_rcv.at[slot, p], partner)

    def source_far():
        for i in range(1, stops):
            z_send(i).start()

    def source():
        mine = x_ref.at[:, own_cols]
        for j in range(1, tp_n):
            t_send(mine, my_slot, j).start()
        p_send(mine, my_slot, tp_i).start()

    def x_stage_a(g, h):
        b = block_of(g, h)
        slot = g * 2 + h

        @pl.when(jnp.logical_and(b % 2 == core, b // 2 != pos))
        def _():
            z_land(slot).wait_recv()
            mine = x_all.at[x_rows(slot, tp_i)]
            for j in range(1, tp_n):
                t_send(mine, slot, j).start()
            p_send(mine, slot, tp_i).start()

    def x_stage_b(g, h):
        b = block_of(g, h)
        slot = g * 2 + h

        @pl.when(b % 2 == core)
        def _():
            for j in range(1, tp_n):
                t_land(slot, j).wait_recv()
                p = (tp_i + tp_n - j) % tp_n
                p_send(x_all.at[x_rows(slot, p)], slot, p).start()

    def x_stage_c(g, h):
        b = block_of(g, h)
        slot = g * 2 + h

        @pl.when(b % 2 != core)
        def _():
            for p in range(tp_n):
                p_land(slot, p).wait_recv()

    def chain_copy(i, h):
        return remote(chain.at[h, i], chain.at[h, i], c_snd.at[h], c_rcv.at[h, i], at_stop(pos + step_of(h)))

    def back_copy(i, h):
        return remote(hid.at[h, i, core], hid.at[h, i, core], h_snd.at[h], h_rcv.at[h, i], at_stop(pos - step_of(h)))

    def side_copy(i, h):
        return remote(hid.at[h, i, core], hid.at[h, i, core], q_snd.at[h], q_rcv.at[h, i], partner)

    def side_land(i, h):
        return remote(hid.at[h, i, 1 - core], hid.at[h, i, 1 - core], q_snd.at[h], q_rcv.at[h, i], partner)

    def inside(i):
        return jnp.logical_and(i >= 0, i < items)

    def multiply(i, h):
        g, c = i // chunks, i % chunks
        rows = pl.ds(pl.multiple_of((g * 2 + h) * block, block), block)
        part[h] = jnp.dot(x_all[rows, :], w_buf[c], preferred_element_type=f32)

    def reduce(i, h):
        done = before(h)

        @pl.when(done == 0)
        def _():
            chain[h, i] = part[h].astype(bf16)

        @pl.when(done > 0)
        def _():
            chain_copy(i, h).wait_recv()

        @pl.when(jnp.logical_and(done > 0, done < stops - 1))
        def _():
            chain[h, i] = (part[h] + chain[h, i].astype(f32)).astype(bf16)

        @pl.when(done < stops - 1)
        def _():
            chain_copy(i, h).start()

        @pl.when(done == stops - 1)
        def _():
            both = part[h] + chain[h, i].astype(f32)
            gate = both[:, :WIDTH]
            hid[h, i, core] = (gate / (1.0 + jnp.exp(-gate)) * both[:, WIDTH:]).astype(bf16)
            back_copy(i, h).start()
            side_copy(i, h).start()

    def relay(i, h):
        done = before(h)

        @pl.when(done < stops - 1)
        def _():
            back_copy(i, h).wait_recv()

            @pl.when(done > 0)
            def _():
                back_copy(i, h).start()

            side_copy(i, h).start()

    def down(i, h):
        side_land(i, h).wait_recv()
        c = i % chunks
        lhs = jnp.concatenate([hid[h, i, 0], hid[h, i, 1]], axis=1)
        tile = min(cols, 2 * WIDTH)
        for n in range(0, cols, tile):
            acc[h, :, n : n + tile] += jnp.dot(lhs, d_buf[c, :, n : n + tile], preferred_element_type=f32)

    def tp_rows(p):
        return pl.ds(pl.multiple_of(p * sub, sub), sub)

    def s_copy(g, j, h):
        return remote(
            stage.at[g, h, tp_rows(peer(j))], got.at[g, h, j - 1], s_snd.at[g, h, j - 1], s_rcv.at[g, h, j - 1],
            (seq_i, peer(j)))

    def f_copy(g, h):
        return remote(
            fin.at[g, h], out_ref.at[seq_i], f_snd.at[g, h], f_rcv.at[seq_i], (block_of(g, h), tp_i))

    def f_land(origin):
        return remote(fin.at[0, 0], out_ref.at[origin], f_snd.at[0, 0], f_rcv.at[origin], (origin, tp_i))

    keep = pltpu.make_async_copy(fin.at[my_g, my_h], out_ref.at[seq_i], o_sem)

    def spread(g, h):
        stage[g, h] = acc[h].astype(bf16)
        acc[h] = jnp.zeros_like(acc[h])
        for j in range(1, tp_n):
            s_copy(g, j, h).start()

    def collect(g, h):
        total = stage[g, h, tp_rows(tp_i), :].astype(f32)
        for j in range(1, tp_n):
            s_copy(g, j, h).wait_recv()
            total = total + got[g, h, j - 1].astype(f32)
        fin[g, h] = total.astype(bf16)

        @pl.when(block_of(g, h) != seq_i)
        def _():
            f_copy(g, h).start()

        @pl.when(block_of(g, h) == seq_i)
        def _():
            keep.start()

    acc[...] = jnp.zeros_like(acc)
    first_use = RS_LAG * jnp.minimum(before(0), before(1))
    far_step = my_g * STAGGER - RELAY_LEAD
    source_step = jnp.maximum(my_g * chunks - SOURCE_LEAD, -RELAY_LEAD)
    prepare_step = jnp.minimum(far_step, source_step)

    def group_starts(s):
        return jnp.logical_and(jnp.logical_and(s >= 0, s < items), s % chunks == 0)

    @pl.loop(0, RELAY_LEAD + items + depth + 2 + OUT_LAG)
    def _(step):
        t = step - RELAY_LEAD
        i_rs = [t - RS_LAG * before(h) for h in range(2)]
        i_ag = [t - rs_depth - AG_LAG * (stops - 1 - before(h)) for h in range(2)]
        i_dn = [i - 1 for i in i_ag]
        i_out = [i - OUT_LAG for i in i_dn]

        @pl.when(t == prepare_step)
        def _():
            prepare()

        @pl.when(t == source_step)
        def _():
            source()

        @pl.when(t == far_step)
        def _():
            source_far()

        for h in range(2):
            s = i_rs[h] + RELAY_LEAD

            @pl.when(group_starts(s))
            def _():
                x_stage_a(s // chunks, h)

        for h in range(2):
            s = i_rs[h] + PARTNER_LEAD

            @pl.when(group_starts(s))
            def _():
                x_stage_b(s // chunks, h)

        @pl.when(jnp.logical_and(t >= first_use, t < first_use + chunks))
        def _():
            c = t - first_use
            for m in range(2):
                w_local(c, m).wait()
                w_land(c, m).wait_recv()

        for h in range(2):
            @pl.when(inside(i_rs[h]))
            def _():
                @pl.when(i_rs[h] % chunks == 0)
                def _():
                    x_stage_c(i_rs[h] // chunks, h)

                multiply(i_rs[h], h)

        for h in range(2):
            @pl.when(inside(i_rs[h]))
            def _():
                reduce(i_rs[h], h)

        for h in range(2):
            @pl.when(inside(i_ag[h]))
            def _():
                relay(i_ag[h], h)

        @pl.when(t == rs_depth + 1)
        def _():
            for q in range(2):
                d_copy(q).wait()

        for h in range(2):
            @pl.when(inside(i_dn[h]))
            def _():
                down(i_dn[h], h)

                @pl.when(i_dn[h] % chunks == chunks - 1)
                def _():
                    spread(i_dn[h] // chunks, h)

            g_out = i_out[h] // chunks
            in_turn = jnp.logical_or(g_out < groups - 1 - held, g_out == groups - 1)

            @pl.when(jnp.logical_and(jnp.logical_and(inside(i_out[h]), i_out[h] % chunks == chunks - 1), in_turn))
            def _():
                collect(g_out, h)

        if held:
            @pl.when(t == items + depth - HELD_LEAD)
            def _():
                for g in range(groups - 1 - held, groups - 1):
                    for h in range(2):
                        collect(g, h)

    for i in range(1, seq_n):
        f_land((seq_i + i) % seq_n).wait_recv()
    keep.wait()

    @pl.when(jnp.logical_and(head, seq_i < seq_n - 1))
    def _():
        edge_copy.wait_send()

    for i in range(1, stops):
        z_send(i).wait_send()

    @pl.loop(0, chunks)
    def _(c):
        for m in range(2):
            w_push(c, m).wait_send()

    @pl.loop(0, groups)
    def _(g):
        for h in range(2):
            slot = g * 2 + h

            @pl.when(block_of(g, h) % 2 == core)
            def _():
                for j in range(1, tp_n):
                    t_land(slot, j).wait_send()
                for p in range(tp_n):
                    p_land(slot, p).wait_send()

            @pl.when(block_of(g, h) != seq_i)
            def _():
                f_copy(g, h).wait_send()

            for j in range(1, tp_n):
                s_copy(g, j, h).wait_send()

    for h in range(2):
        done = before(h)
        remote(hid.at[h, :, core], hid.at[h, :, core], q_snd.at[h], q_rcv.at[h, 0], partner).wait_send()

        @pl.when(done < stops - 1)
        def _():
            remote(chain.at[h], chain.at[h], c_snd.at[h], c_rcv.at[h, 0], partner).wait_send()

        @pl.when(done > 0)
        def _():
            remote(hid.at[h, :, core], hid.at[h, :, core], h_snd.at[h], h_rcv.at[h, 0], partner).wait_send()


def shards(tokens, conv_weight, norm_gain, gate_weight, up_weight, down_weight):
    seq_n, tp_n = lax.axis_size("seq"), lax.axis_size("tp")
    block, width = tokens.shape
    sub = block // tp_n
    feats, units = gate_weight.shape
    cols = down_weight.shape[1]
    stops = groups = seq_n // 2
    chunks = units // (2 * WIDTH)
    n = groups * chunks
    slots = 2 * groups
    bf16, f32 = jnp.bfloat16, jnp.float32
    dma = pltpu.SemaphoreType.DMA
    vmem = pl.BlockSpec(memory_space=pltpu.VMEM)
    anywhere = pl.BlockSpec(memory_space=pl.ANY)
    pieces = pl.pallas_call(
        functools.partial(ffn_kernel, seq_n, tp_n),
        out_shape=pltpu.VMEM((seq_n, sub, cols), bf16),
        in_specs=[anywhere, anywhere, anywhere, anywhere, anywhere, anywhere],
        out_specs=vmem,
        scratch_shapes=[
            pltpu.VMEM(conv_weight.shape, f32),
            pltpu.VMEM((1, width), f32),
            pltpu.VMEM((EDGE + sub, width), bf16),
            pltpu.VMEM((EDGE, width), bf16),
            pltpu.VMEM((sub, width), f32),
            pltpu.VMEM((sub, width), bf16),
            pltpu.VMEM((slots * block, 2 * feats), bf16),
            pltpu.VMEM((chunks, 2 * feats, 2 * WIDTH), bf16),
            pltpu.VMEM((chunks, 2 * WIDTH, cols), bf16),
            pltpu.VMEM((2, n, block, 2 * WIDTH), bf16),
            pltpu.VMEM((2, n, 2, block, WIDTH), bf16),
            pltpu.VMEM((2, block, 2 * WIDTH), f32),
            pltpu.VMEM((2, block, cols), f32),
            pltpu.VMEM((groups, 2, block, cols), bf16),
            pltpu.VMEM((groups, 2, tp_n - 1, sub, cols), bf16),
            pltpu.VMEM((groups, 2, sub, cols), bf16),
            dma(()), dma(()), dma(()), dma(()), dma(()), dma(()), dma(()),
            dma((chunks, 2)), dma((chunks, 2)), dma((chunks, 2)), dma((2,)),
            dma((stops - 1,)), dma((slots,)), dma((slots, tp_n - 1)), dma((slots, tp_n - 1)),
            dma((slots, tp_n)), dma((slots, tp_n)),
            dma((2,)), dma((2, n)), dma((2,)), dma((2, n)), dma((2,)), dma((2, n)),
            dma((groups, 2, tp_n - 1)), dma((groups, 2, tp_n - 1)), dma((groups, 2)), dma((seq_n,)),
        ],
        compiler_params=pltpu.CompilerParams(
            collective_id=0, has_side_effects=True, vmem_limit_bytes=60 * 1024 * 1024),
        cost_estimate=pl.CostEstimate(
            flops=6 * slots * block * feats * units, bytes_accessed=6 * feats * units, transcendentals=0),
    )(conv_weight, norm_gain.reshape(1, width), tokens, gate_weight, up_weight,
      down_weight.reshape(2, chunks, WIDTH, cols))
    return jnp.transpose(pieces, (1, 0, 2)).reshape(sub, seq_n * cols)


def solution(mesh):
    in_specs = (P("seq", None), P(), P(), P("seq", "tp"), P("seq", "tp"), P("tp", "seq"))
    out_specs = P(("seq", "tp"), None)
    return jax.shard_map(shards, mesh=mesh, in_specs=in_specs, out_specs=out_specs, check_vma=False)
```

```python
import functools

import jax
import jax.numpy as jnp
from jax import lax
from jax.experimental import pallas as pl
from jax.experimental.pallas import tpu as pltpu
from jax.sharding import PartitionSpec as P

MESH = pl.DeviceIdType.MESH
WIDTH = 128
RS_LAG = 3
AG_LAG = 3
SOURCE_LEAD = 10
RELAY_LEAD = 6
STAGGER = 1
EDGE = 16
CONV_TILE = 1024
PARTNER_LEAD = 1
OUT_LAG = 5
HELD = 3
HELD_LEAD = 3


def ffn_kernel(seq_n, tp_n, taps_hbm, gain_hbm, tok_ref, gw_ref, uw_ref, dw_ref, out_ref,
               taps_ref, gain_ref, tok, edge, conv, x_ref, x_all, w_buf, d_buf, chain, hid, part, acc, stage, got, fin,
               taps_sem, gain_sem, tok_sem, edge_sem, e_snd, e_rcv, o_sem, w_sem, w_snd, w_rcv, d_sem, z_snd, z_rcv, t_snd, t_rcv, p_snd, p_rcv,
               c_snd, c_rcv, h_snd, h_rcv, q_snd, q_rcv, s_snd, s_rcv, f_snd, f_rcv):
    stops = seq_n // 2
    groups = seq_n // 2
    seq_i = lax.axis_index("seq")
    tp_i = lax.axis_index("tp")
    pos = seq_i // 2
    core = seq_i % 2
    partner = (pos * 2 + 1 - core, tp_i)
    sub, width = x_ref.shape
    block = sub * tp_n
    span = width // stops
    feats = span // 2
    units = gw_ref.shape[1]
    own_units = units // 2
    chunks = own_units // WIDTH
    items = groups * chunks
    cols = d_buf.shape[2]
    rs_depth = RS_LAG * (stops - 1)
    depth = rs_depth + AG_LAG * (stops - 1)
    held = min(HELD, groups - 1)
    bf16, f32 = jnp.bfloat16, jnp.float32

    my_h = jnp.where(seq_i < groups, 1, 0)
    my_g = jnp.where(seq_i < groups, seq_i, seq_n - 1 - seq_i)
    my_slot = my_g * 2 + my_h

    def block_of(g, h):
        return seq_n - 1 - g if h == 0 else g

    def before(h):
        return stops - 1 - pos if h == 0 else pos

    def step_of(h):
        return -1 if h == 0 else 1

    def at_stop(stop):
        return (stop * 2 + core, tp_i)

    def peer(j):
        return (tp_i + j) % tp_n

    def x_rows(slot, p):
        return pl.ds(pl.multiple_of(slot * block + p * sub, sub), sub)

    def remote(src, dst, snd, rcv, dev):
        return pltpu.make_async_remote_copy(
            src_ref=src, dst_ref=dst, send_sem=snd, recv_sem=rcv, device_id=dev, device_id_type=MESH)

    k_rows = pl.ds(pl.multiple_of(core * feats, feats), feats)
    up_gate = (gw_ref, uw_ref)

    def w_cols(q, c):
        return pl.ds(pl.multiple_of(q * own_units + c * WIDTH, WIDTH), WIDTH)

    def w_local(c, m):
        return pltpu.make_async_copy(
            up_gate[m].at[:, w_cols(core, c)], w_buf.at[c, k_rows, pl.ds(m * WIDTH, WIDTH)], w_sem.at[c, m])

    def w_push(c, m):
        return remote(
            up_gate[m].at[:, w_cols(1 - core, c)], w_buf.at[c, k_rows, pl.ds(m * WIDTH, WIDTH)],
            w_snd.at[c, m], w_rcv.at[c, m], partner)

    def w_land(c, m):
        there = pl.ds(pl.multiple_of((1 - core) * feats, feats), feats)
        return remote(
            up_gate[m].at[:, w_cols(core, c)], w_buf.at[c, there, pl.ds(m * WIDTH, WIDTH)],
            w_snd.at[c, m], w_rcv.at[c, m], partner)

    def d_copy(q):
        return pltpu.make_async_copy(dw_ref.at[q], d_buf.at[:, pl.ds(q * WIDTH, WIDTH)], d_sem.at[q])

    taps_copy = pltpu.make_async_copy(taps_hbm, taps_ref, taps_sem)
    gain_copy = pltpu.make_async_copy(gain_hbm, gain_ref, gain_sem)
    taps_copy.start()
    gain_copy.start()
    head = tp_i == 0
    body = pltpu.make_async_copy(
        tok_ref.at[pl.ds(0, sub)], tok.at[pl.ds(EDGE, sub)], tok_sem)
    with_edge = pltpu.make_async_copy(
        tok_ref.at[pl.ds(pl.multiple_of(jnp.maximum(tp_i * sub - EDGE, 0), EDGE), EDGE + sub)], tok, tok_sem)
    tail = pltpu.make_async_copy(tok_ref.at[pl.ds(block - EDGE, EDGE)], edge, edge_sem)
    edge_copy = remote(edge, tok.at[pl.ds(0, EDGE)], e_snd, e_rcv, ((seq_i + 1) % seq_n, tp_i))

    @pl.when(head)
    def _():
        body.start()
        tail.start()

    @pl.when(jnp.logical_not(head))
    def _():
        with_edge.start()

    @pl.loop(0, chunks)
    def _(c):
        for m in range(2):
            w_local(c, m).start()

    barrier = pltpu.get_barrier_semaphore()
    for i in range(1, seq_n):
        pl.semaphore_signal(barrier, inc=1, device_id=((seq_i + i) % seq_n, tp_i), device_id_type=MESH)
    for j in range(1, tp_n):
        pl.semaphore_signal(barrier, inc=1, device_id=(seq_i, peer(j)), device_id_type=MESH)

    def normalize():
        taps_copy.wait()
        gain_copy.wait()
        n_taps = taps_ref.shape[0]

        def convolve(n, squares):
            at = pl.ds(pl.multiple_of(n * CONV_TILE, CONV_TILE), CONV_TILE)
            rows = tok[:, at].astype(f32)
            total = jnp.zeros((sub, CONV_TILE), f32)
            for k in range(n_taps):
                moved = pltpu.roll(rows, k, 0) if k else rows
                total = total + taps_ref[k : k + 1, at] * moved[EDGE:]
            conv[:, at] = total
            return squares + jnp.sum(total * total, axis=1, keepdims=True)

        squares = lax.fori_loop(0, width // CONV_TILE, convolve, jnp.zeros((sub, 1), f32))
        scale = lax.rsqrt(squares / width + 1e-05)

        @pl.loop(0, width // CONV_TILE)
        def _(n):
            at = pl.ds(pl.multiple_of(n * CONV_TILE, CONV_TILE), CONV_TILE)
            x_ref[:, at] = (conv[:, at] * scale * gain_ref[:, at]).astype(bf16)

    @pl.when(jnp.logical_not(head))
    def _():
        with_edge.wait()
        normalize()

    pl.semaphore_wait(barrier, seq_n + tp_n - 2)

    @pl.when(jnp.logical_and(head, seq_i < seq_n - 1))
    def _():
        tail.wait()
        edge_copy.start()

    @pl.when(jnp.logical_and(head, seq_i == seq_n - 1))
    def _():
        tail.wait()

    @pl.loop(0, chunks)
    def _(c):
        for m in range(2):
            w_push(c, m).start()

    for q in range(2):
        d_copy(q).start()

    def prepare():
        @pl.when(head)
        def _():
            body.wait()

            @pl.when(seq_i == 0)
            def _():
                tok[0:EDGE, :] = jnp.zeros((EDGE, width), bf16)

            @pl.when(seq_i > 0)
            def _():
                edge_copy.wait_recv()

            normalize()

        x_all[x_rows(my_slot, tp_i), :] = x_ref[:, own_cols]

    own_cols = pl.ds(pl.multiple_of(pos * span, span), span)

    def z_stop(i):
        return (pos + jnp.where(my_h == 1, i, stops - i)) % stops

    def z_send(i):
        stop = z_stop(i)
        return remote(
            x_ref.at[:, pl.ds(pl.multiple_of(stop * span, span), span)], x_all.at[x_rows(my_slot, tp_i)],
            z_snd.at[i - 1], z_rcv.at[my_slot], at_stop(stop))

    def z_land(slot):
        return remote(
            x_ref.at[:, own_cols], x_all.at[x_rows(slot, tp_i)], z_snd.at[0], z_rcv.at[slot], at_stop((pos + 1) % stops))

    def t_send(src, slot, j):
        return remote(
            src, x_all.at[x_rows(slot, tp_i)], t_snd.at[slot, j - 1], t_rcv.at[slot, j - 1], (seq_i, peer(j)))

    def t_land(slot, j):
        rows = x_all.at[x_rows(slot, (tp_i + tp_n - j) % tp_n)]
        return remote(rows, rows, t_snd.at[slot, j - 1], t_rcv.at[slot, j - 1], (seq_i, peer(j)))

    def p_send(src, slot, p):
        return remote(src, x_all.at[x_rows(slot, p)], p_snd.at[slot, p], p_rcv.at[slot, p], partner)

    def p_land(slot, p):
        rows = x_all.at[x_rows(slot, p)]
        return remote(rows, rows, p_snd.at[slot, p], p_rcv.at[slot, p], partner)

    def source_far():
        for i in range(1, stops):
            z_send(i).start()

    def source():
        mine = x_ref.at[:, own_cols]
        for j in range(1, tp_n):
            t_send(mine, my_slot, j).start()
        p_send(mine, my_slot, tp_i).start()

    def x_stage_a(g, h):
        b = block_of(g, h)
        slot = g * 2 + h

        @pl.when(jnp.logical_and(b % 2 == core, b // 2 != pos))
        def _():
            z_land(slot).wait_recv()
            mine = x_all.at[x_rows(slot, tp_i)]
            for j in range(1, tp_n):
                t_send(mine, slot, j).start()
            p_send(mine, slot, tp_i).start()

    def x_stage_b(g, h):
        b = block_of(g, h)
        slot = g * 2 + h

        @pl.when(b % 2 == core)
        def _():
            for j in range(1, tp_n):
                t_land(slot, j).wait_recv()
                p = (tp_i + tp_n - j) % tp_n
                p_send(x_all.at[x_rows(slot, p)], slot, p).start()

    def x_stage_c(g, h):
        b = block_of(g, h)
        slot = g * 2 + h

        @pl.when(b % 2 != core)
        def _():
            for p in range(tp_n):
                p_land(slot, p).wait_recv()

    def chain_copy(i, h):
        return remote(chain.at[h, i], chain.at[h, i], c_snd.at[h], c_rcv.at[h, i], at_stop(pos + step_of(h)))

    def back_copy(i, h):
        return remote(hid.at[h, i, core], hid.at[h, i, core], h_snd.at[h], h_rcv.at[h, i], at_stop(pos - step_of(h)))

    def side_copy(i, h):
        return remote(hid.at[h, i, core], hid.at[h, i, core], q_snd.at[h], q_rcv.at[h, i], partner)

    def side_land(i, h):
        return remote(hid.at[h, i, 1 - core], hid.at[h, i, 1 - core], q_snd.at[h], q_rcv.at[h, i], partner)

    def inside(i):
        return jnp.logical_and(i >= 0, i < items)

    def multiply(i, h):
        g, c = i // chunks, i % chunks
        rows = pl.ds(pl.multiple_of((g * 2 + h) * block, block), block)
        part[h] = jnp.dot(x_all[rows, :], w_buf[c], preferred_element_type=f32)

    def reduce(i, h):
        done = before(h)

        @pl.when(done == 0)
        def _():
            chain[h, i] = part[h].astype(bf16)

        @pl.when(done > 0)
        def _():
            chain_copy(i, h).wait_recv()

        @pl.when(jnp.logical_and(done > 0, done < stops - 1))
        def _():
            chain[h, i] = (part[h] + chain[h, i].astype(f32)).astype(bf16)

        @pl.when(done < stops - 1)
        def _():
            chain_copy(i, h).start()

        @pl.when(done == stops - 1)
        def _():
            both = part[h] + chain[h, i].astype(f32)
            gate = both[:, :WIDTH]
            hid[h, i, core] = (gate / (1.0 + jnp.exp(-gate)) * both[:, WIDTH:]).astype(bf16)
            back_copy(i, h).start()
            side_copy(i, h).start()

    def relay(i, h):
        done = before(h)

        @pl.when(done < stops - 1)
        def _():
            back_copy(i, h).wait_recv()

            @pl.when(done > 0)
            def _():
                back_copy(i, h).start()

            side_copy(i, h).start()

    def down(i, h):
        side_land(i, h).wait_recv()
        c = i % chunks
        lhs = jnp.concatenate([hid[h, i, 0], hid[h, i, 1]], axis=1)
        tile = min(cols, 2 * WIDTH)
        for n in range(0, cols, tile):
            acc[h, :, n : n + tile] += jnp.dot(lhs, d_buf[c, :, n : n + tile], preferred_element_type=f32)

    def tp_rows(p):
        return pl.ds(pl.multiple_of(p * sub, sub), sub)

    def s_copy(g, j, h):
        return remote(
            stage.at[g, h, tp_rows(peer(j))], got.at[g, h, j - 1], s_snd.at[g, h, j - 1], s_rcv.at[g, h, j - 1],
            (seq_i, peer(j)))

    def f_copy(g, h):
        return remote(
            fin.at[g, h], out_ref.at[seq_i], f_snd.at[g, h], f_rcv.at[seq_i], (block_of(g, h), tp_i))

    def f_land(origin):
        return remote(fin.at[0, 0], out_ref.at[origin], f_snd.at[0, 0], f_rcv.at[origin], (origin, tp_i))

    keep = pltpu.make_async_copy(fin.at[my_g, my_h], out_ref.at[seq_i], o_sem)

    def spread(g, h):
        stage[g, h] = acc[h].astype(bf16)
        acc[h] = jnp.zeros_like(acc[h])
        for j in range(1, tp_n):
            s_copy(g, j, h).start()

    def collect(g, h):
        total = stage[g, h, tp_rows(tp_i), :].astype(f32)
        for j in range(1, tp_n):
            s_copy(g, j, h).wait_recv()
            total = total + got[g, h, j - 1].astype(f32)
        fin[g, h] = total.astype(bf16)

    def deliver(g, h):
        @pl.when(block_of(g, h) != seq_i)
        def _():
            f_copy(g, h).start()

        @pl.when(block_of(g, h) == seq_i)
        def _():
            keep.start()

    acc[...] = jnp.zeros_like(acc)
    first_use = RS_LAG * jnp.minimum(before(0), before(1))
    far_step = my_g * STAGGER - RELAY_LEAD
    source_step = jnp.maximum(my_g * chunks - SOURCE_LEAD, -RELAY_LEAD)
    prepare_step = jnp.minimum(far_step, source_step)

    def group_starts(s):
        return jnp.logical_and(jnp.logical_and(s >= 0, s < items), s % chunks == 0)

    @pl.loop(0, RELAY_LEAD + items + depth + 2 + OUT_LAG)
    def _(step):
        t = step - RELAY_LEAD
        i_rs = [t - RS_LAG * before(h) for h in range(2)]
        i_ag = [t - rs_depth - AG_LAG * (stops - 1 - before(h)) for h in range(2)]
        i_dn = [i - 1 for i in i_ag]
        i_out = [i - OUT_LAG for i in i_dn]

        @pl.when(t == prepare_step)
        def _():
            prepare()

        @pl.when(t == source_step)
        def _():
            source()

        @pl.when(t == far_step)
        def _():
            source_far()

        for h in range(2):
            s = i_rs[h] + RELAY_LEAD

            @pl.when(group_starts(s))
            def _():
                x_stage_a(s // chunks, h)

        for h in range(2):
            s = i_rs[h] + PARTNER_LEAD

            @pl.when(group_starts(s))
            def _():
                x_stage_b(s // chunks, h)

        @pl.when(jnp.logical_and(t >= first_use, t < first_use + chunks))
        def _():
            c = t - first_use
            for m in range(2):
                w_local(c, m).wait()
                w_land(c, m).wait_recv()

        for h in range(2):
            @pl.when(inside(i_rs[h]))
            def _():
                @pl.when(i_rs[h] % chunks == 0)
                def _():
                    x_stage_c(i_rs[h] // chunks, h)

                multiply(i_rs[h], h)

        for h in range(2):
            @pl.when(inside(i_rs[h]))
            def _():
                reduce(i_rs[h], h)

        for h in range(2):
            @pl.when(inside(i_ag[h]))
            def _():
                relay(i_ag[h], h)

        @pl.when(t == rs_depth + 1)
        def _():
            for q in range(2):
                d_copy(q).wait()

        for h in range(2):
            @pl.when(inside(i_dn[h]))
            def _():
                down(i_dn[h], h)

                @pl.when(i_dn[h] % chunks == chunks - 1)
                def _():
                    spread(i_dn[h] // chunks, h)

            g_out = i_out[h] // chunks
            in_turn = jnp.logical_or(g_out < groups - 1 - held, g_out == groups - 1)

            @pl.when(jnp.logical_and(inside(i_out[h]), i_out[h] % chunks == chunks - 1))
            def _():
                collect(g_out, h)

                @pl.when(in_turn)
                def _():
                    deliver(g_out, h)

        if held:
            @pl.when(t == items + depth - min(HELD_LEAD, chunks - OUT_LAG))
            def _():
                for g in range(groups - 1 - held, groups - 1):
                    for h in range(2):
                        deliver(g, h)

    for i in range(1, seq_n):
        f_land((seq_i + i) % seq_n).wait_recv()
    keep.wait()

    @pl.when(jnp.logical_and(head, seq_i < seq_n - 1))
    def _():
        edge_copy.wait_send()

    for i in range(1, stops):
        z_send(i).wait_send()

    @pl.loop(0, chunks)
    def _(c):
        for m in range(2):
            w_push(c, m).wait_send()

    @pl.loop(0, groups)
    def _(g):
        for h in range(2):
            slot = g * 2 + h

            @pl.when(block_of(g, h) % 2 == core)
            def _():
                for j in range(1, tp_n):
                    t_land(slot, j).wait_send()
                for p in range(tp_n):
                    p_land(slot, p).wait_send()

            @pl.when(block_of(g, h) != seq_i)
            def _():
                f_copy(g, h).wait_send()

            for j in range(1, tp_n):
                s_copy(g, j, h).wait_send()

    for h in range(2):
        done = before(h)
        remote(hid.at[h, :, core], hid.at[h, :, core], q_snd.at[h], q_rcv.at[h, 0], partner).wait_send()

        @pl.when(done < stops - 1)
        def _():
            remote(chain.at[h], chain.at[h], c_snd.at[h], c_rcv.at[h, 0], partner).wait_send()

        @pl.when(done > 0)
        def _():
            remote(hid.at[h, :, core], hid.at[h, :, core], h_snd.at[h], h_rcv.at[h, 0], partner).wait_send()


def shards(tokens, conv_weight, norm_gain, gate_weight, up_weight, down_weight):
    seq_n, tp_n = lax.axis_size("seq"), lax.axis_size("tp")
    block, width = tokens.shape
    sub = block // tp_n
    feats, units = gate_weight.shape
    cols = down_weight.shape[1]
    stops = groups = seq_n // 2
    chunks = units // (2 * WIDTH)
    n = groups * chunks
    slots = 2 * groups
    bf16, f32 = jnp.bfloat16, jnp.float32
    dma = pltpu.SemaphoreType.DMA
    vmem = pl.BlockSpec(memory_space=pltpu.VMEM)
    anywhere = pl.BlockSpec(memory_space=pl.ANY)
    pieces = pl.pallas_call(
        functools.partial(ffn_kernel, seq_n, tp_n),
        out_shape=pltpu.VMEM((seq_n, sub, cols), bf16),
        in_specs=[anywhere, anywhere, anywhere, anywhere, anywhere, anywhere],
        out_specs=vmem,
        scratch_shapes=[
            pltpu.VMEM(conv_weight.shape, f32),
            pltpu.VMEM((1, width), f32),
            pltpu.VMEM((EDGE + sub, width), bf16),
            pltpu.VMEM((EDGE, width), bf16),
            pltpu.VMEM((sub, width), f32),
            pltpu.VMEM((sub, width), bf16),
            pltpu.VMEM((slots * block, 2 * feats), bf16),
            pltpu.VMEM((chunks, 2 * feats, 2 * WIDTH), bf16),
            pltpu.VMEM((chunks, 2 * WIDTH, cols), bf16),
            pltpu.VMEM((2, n, block, 2 * WIDTH), bf16),
            pltpu.VMEM((2, n, 2, block, WIDTH), bf16),
            pltpu.VMEM((2, block, 2 * WIDTH), f32),
            pltpu.VMEM((2, block, cols), f32),
            pltpu.VMEM((groups, 2, block, cols), bf16),
            pltpu.VMEM((groups, 2, tp_n - 1, sub, cols), bf16),
            pltpu.VMEM((groups, 2, sub, cols), bf16),
            dma(()), dma(()), dma(()), dma(()), dma(()), dma(()), dma(()),
            dma((chunks, 2)), dma((chunks, 2)), dma((chunks, 2)), dma((2,)),
            dma((stops - 1,)), dma((slots,)), dma((slots, tp_n - 1)), dma((slots, tp_n - 1)),
            dma((slots, tp_n)), dma((slots, tp_n)),
            dma((2,)), dma((2, n)), dma((2,)), dma((2, n)), dma((2,)), dma((2, n)),
            dma((groups, 2, tp_n - 1)), dma((groups, 2, tp_n - 1)), dma((groups, 2)), dma((seq_n,)),
        ],
        compiler_params=pltpu.CompilerParams(
            collective_id=0, has_side_effects=True, vmem_limit_bytes=60 * 1024 * 1024),
        cost_estimate=pl.CostEstimate(
            flops=6 * slots * block * feats * units, bytes_accessed=6 * feats * units, transcendentals=0),
    )(conv_weight, norm_gain.reshape(1, width), tokens, gate_weight, up_weight,
      down_weight.reshape(2, chunks, WIDTH, cols))
    return jnp.transpose(pieces, (1, 0, 2)).reshape(sub, seq_n * cols)


def solution(mesh):
    in_specs = (P("seq", None), P(), P(), P("seq", "tp"), P("seq", "tp"), P("tp", "seq"))
    out_specs = P(("seq", "tp"), None)
    return jax.shard_map(shards, mesh=mesh, in_specs=in_specs, out_specs=out_specs, check_vma=False)
```
